256 devices in a mesh: bank: 64 (over z, y, core), zero: 4 (over x).
Axes of the slice: x: 4, y: 4, z: 8, core: 2. Of those that a mesh axis runs over, the one named last changes fastest.
Arguments:
- w_gate: float32 [64, 2048, 1024], P('bank', 'zero'), may hold values from -0.1875 to 0.1875
- avg_gate: float32 [64, 2048, 1024], P('bank', 'zero'), may hold values from -0.125 to 0.125
- w_up: float32 [64, 2048, 1024], P('bank', 'zero'), may hold values from -0.1875 to 0.1875
- avg_up: float32 [64, 2048, 1024], P('bank', 'zero'), may hold values from -0.125 to 0.125
- mix_share: float32 [64], P('bank'), may hold values from 0.2 to 0.8
- router_weight: float32 [2048, 64], P('zero', 'bank'), may hold values from -0.125 to 0.125
- router_gain: float32 [2048], P('zero'), may hold values from 0.25 to 1.75
Outputs:
- serve_gate: bfloat16 [64, 2048, 1024], P('bank')
- serve_up: bfloat16 [64, 2048, 1024], P('bank')
- scale_gate: float32 [64, 1024], P('bank')
- scale_up: float32 [64, 1024], P('bank')
- serve_router: bfloat16 [2048, 64], replicated
The draws below stay inside these ranges and needn't reach their ends.
All inputs are finite; a program needn't handle non-finite values.
Results may differ from the reference program's by a relative error of at most 0.001.
Values may be sent and summed in bfloat16 or wider, within the bound.
A program may use at most 64 MiB of HBM per device.

```python
import jax
import jax.numpy as jnp
from jax import lax

EXPERTS = 64
D_MODEL = 2048
D_EXPERT = 1024


def spiked(values, rng, source, target, blocks, factor):
    owner, partner = [(jnp.arange(values.shape[axis_at]) // (values.shape[axis_at] // blocks)).reshape([-1 if axis == axis_at else 1 for axis in range(values.ndim)]) for axis_at in (source, target)]
    chosen = jax.random.permutation(rng, blocks)[partner]
    strong = (owner == chosen) | (owner == (partner + blocks // 2) % blocks)
    return jnp.where(strong, factor * values, values)


def block_levels(own_key, dims, shards, low, high):
    gain, own = 1.0, jax.random.fold_in(own_key, 6)
    for axis_at, parts in shards:
        draws = jnp.exp(jax.random.uniform(jax.random.fold_in(own, axis_at), (parts,), jnp.float32, low / len(shards), high / len(shards)))
        gain = gain * jnp.repeat(draws, dims[axis_at] // parts).reshape([-1 if axis == axis_at else 1 for axis in range(len(dims))])
    return gain


def scatter_about(key, shape, width, bound, split=(), kind=jnp.bfloat16):
    level = block_levels(key, shape, split, -0.22, 0.18) if split else 1.0
    array = jax.random.normal(key, shape, jnp.float32) * width * level
    return jnp.minimum(jnp.maximum(array, -bound), bound).astype(kind)


def noise_with(stream_key, extent, spread, reach, pieces, heavy, dtype=jnp.bfloat16):
    values = spread * jax.random.normal(stream_key, extent, jnp.float32)
    if pieces:
        values = values * block_levels(stream_key, extent, pieces, -0.22, 0.18)
    return jnp.clip(spiked(values, jax.random.fold_in(stream_key, 3), *heavy), -reach, reach).astype(dtype)


def setup_inputs(seed: int = 0) -> dict:
    splits = jax.random.split(jax.random.key(seed), 8)
    return {
        "w_gate": noise_with(splits[0], (EXPERTS, D_MODEL, D_EXPERT), D_MODEL ** -0.5, 0.1875, ((0, 64), (1, 4)), (1, 2, 4, 2.0), jnp.float32),
        "avg_gate": scatter_about(splits[1], (EXPERTS, D_MODEL, D_EXPERT), D_MODEL ** -0.5, 0.125, ((0, 64), (1, 4)), jnp.float32),
        "w_up": noise_with(splits[2], (EXPERTS, D_MODEL, D_EXPERT), D_MODEL ** -0.5, 0.1875, ((0, 64), (1, 4)), (1, 2, 4, 2.0), jnp.float32),
        "avg_up": scatter_about(splits[3], (EXPERTS, D_MODEL, D_EXPERT), D_MODEL ** -0.5, 0.125, ((0, 64), (1, 4)), jnp.float32),
        "mix_share": jnp.clip(0.2 + 0.6 * jax.random.uniform(splits[4], (EXPERTS,), jnp.float32) ** block_levels(splits[4], (EXPERTS,), ((0, 64),), -0.2, 0.2), 0.2, 0.8),
        "router_weight": scatter_about(splits[5], (D_MODEL, EXPERTS), D_MODEL ** -0.5, 0.125, ((0, 4), (1, 64)), jnp.float32),
        "router_gain": jnp.clip(1.0 + 0.15 * jax.random.normal(splits[6], (D_MODEL,), jnp.float32), 0.25, 1.75),
    }


def reference(w_gate, avg_gate, w_up, avg_up, mix_share, router_weight, router_gain):
    fresh_gate = mix_share[:, None, None] * w_gate + (1.0 - mix_share[:, None, None]) * avg_gate
    fresh_up = mix_share[:, None, None] * w_up + (1.0 - mix_share[:, None, None]) * avg_up
    scale_gate = jnp.sqrt(lax.optimization_barrier(jnp.sum(fresh_gate * fresh_gate, axis=1)))
    serve_gate = (fresh_gate / jnp.expand_dims(scale_gate, 1)).astype(jnp.bfloat16)
    scale_up = jnp.sqrt(lax.optimization_barrier(jnp.sum(fresh_up * fresh_up, axis=1)))
    serve_up = (fresh_up / jnp.expand_dims(scale_up, 1)).astype(jnp.bfloat16)
    serve_router = (router_weight * router_gain[:, None]).astype(jnp.bfloat16)
    return (serve_gate, serve_up, scale_gate, scale_up, serve_router)
```

```python
import jax
import jax.numpy as jnp
from jax import lax
from jax.experimental import pallas as pl
from jax.experimental.pallas import tpu as pltpu
from jax.sharding import PartitionSpec as P

MESH = pl.DeviceIdType.MESH
ROWS = 512
COLS = 1024
WIDTH = 256
PER = COLS // WIDTH
CHUNKS = 2 * PER
STEP = 64
RB = 16


def kernel(
    w_gate, avg_gate, w_up, avg_up, mix, router_w, router_g,
    o_gate, o_up, o_sgate, o_sup, o_router,
    wide, other, wide_sem, other_sem, mix_s, mix_sem, rw, rg, rw_sem, rg_sem,
    sums0, sums1, scale, sums_send, sums_recv,
    narrow, send_r, send_l, recv_l, recv_r, fsend, frecv, put, put_far,
    xr, bank_r, out_r, rx_send, rx_recv, rc, ry, rz, small,
):
    bank = lax.axis_index("bank")
    me = lax.axis_index("zero")
    right, left, across = lax.rem(me + 1, 4), lax.rem(me + 3, 4), lax.rem(me + 2, 4)
    core = lax.rem(bank, 2)
    yy = lax.rem(bank // 2, 4)
    zz = bank // 8

    def at_bank(z, y, c):
        return (z * 4 + y) * 2 + c

    twin = at_bank(zz, yy, 1 - core)
    y_up, y_down = at_bank(zz, lax.rem(yy + 1, 4), core), at_bank(zz, lax.rem(yy + 3, 4), core)
    z_up, z_down = at_bank(lax.rem(zz + 1, 8), yy, core), at_bank(lax.rem(zz + 7, 8), yy, core)

    w_in, a_in = (w_gate, w_up), (avg_gate, avg_up)

    mix_copy = pltpu.make_async_copy(mix, mix_s, mix_sem)
    mix_copy.start()
    loads = []
    for c in range(CHUNKS):
        m, cols = c // PER, pl.ds((c % PER) * WIDTH, WIDTH)
        first = pltpu.make_async_copy(w_in[m].at[:, cols], wide.at[c], wide_sem.at[c])
        second = pltpu.make_async_copy(a_in[m].at[:, cols], other.at[c], other_sem.at[c])
        first.start()
        second.start()
        loads.append((first, second))
    load_rw = pltpu.make_async_copy(router_w, rw, rw_sem)
    load_rg = pltpu.make_async_copy(router_g, rg, rg_sem)
    load_rw.start()
    load_rg.start()

    barrier = pltpu.get_barrier_semaphore()
    for where in (
        (bank, right), (bank, left), (bank, across),
        (twin, me), (y_up, me), (y_down, me), (z_up, me), (z_down, me),
    ):
        pl.semaphore_signal(barrier, inc=1, device_id=where, device_id_type=MESH)

    mix_copy.wait()
    share = mix_s[0]
    rest = 1.0 - share

    def mixed(c):
        loads[c][0].wait()
        loads[c][1].wait()

        def step(i, acc):
            rows = pl.ds(i * STEP, STEP)
            fresh = share * wide[c, rows, :] + rest * other[c, rows, :]
            wide[c, rows, :] = fresh
            return acc + jnp.sum((fresh * fresh).reshape(STEP // 8, 8, WIDTH), axis=0)

        acc = lax.fori_loop(0, ROWS // STEP, step, jnp.zeros((8, WIDTH), jnp.float32))
        return jnp.sum(acc, axis=0, keepdims=True)

    peers = (right, left, across)

    def share_sums(buf, g):
        copies = []
        for k, peer in enumerate(peers):
            copy = pltpu.make_async_remote_copy(
                src_ref=buf.at[me], dst_ref=buf.at[me],
                send_sem=sums_send.at[g, k], recv_sem=sums_recv.at[g, k],
                device_id=(bank, peer), device_id_type=MESH,
            )
            copy.start()
            copies.append(copy)
        return copies

    sums0[me] = mixed(0)
    pl.semaphore_wait(barrier, 8)
    sent0 = share_sums(sums0, 0)

    load_rw.wait()
    load_rg.wait()
    prod = rw[...] * rg[...]
    for k in range(4):
        xr[me, pl.ds(k, 1), :] = prod[:, k * 128 : (k + 1) * 128]
    sent_x = []
    for k, peer in enumerate(peers):
        copy = pltpu.make_async_remote_copy(
            src_ref=xr.at[me], dst_ref=xr.at[me],
            send_sem=rx_send.at[k], recv_sem=rx_recv.at[k],
            device_id=(bank, peer), device_id_type=MESH,
        )
        copy.start()
        sent_x.append(copy)

    for c in range(1, CHUNKS):
        sums1[me, :, pl.ds((c - 1) * WIDTH, WIDTH)] = mixed(c)
    sent1 = share_sums(sums1, 1)

    def where_at(c, owner):
        return narrow.at[c // PER, pl.ds(owner * ROWS, ROWS), pl.ds((c % PER) * WIDTH, WIDTH)]

    def out_at(c, owner):
        return (o_gate, o_up)[c // PER].at[pl.ds(owner * ROWS, ROWS), pl.ds((c % PER) * WIDTH, WIDTH)]

    def write(c, owner, sem):
        copy = pltpu.make_async_copy(where_at(c, owner), out_at(c, owner), sem)
        copy.start()
        writes.append(copy)

    writes = []
    sent = []

    def normalised(c):
        s = scale[c // PER, :, pl.ds((c % PER) * WIDTH, WIDTH)]
        inverse = 1.0 / s

        def step(i, carry):
            rows = pl.ds(i * STEP, STEP)
            narrow[
                c // PER, pl.ds(pl.multiple_of(me * ROWS + i * STEP, STEP), STEP),
                pl.ds((c % PER) * WIDTH, WIDTH),
            ] = (wide[c, rows, :] * inverse).astype(jnp.bfloat16)
            return carry

        lax.fori_loop(0, ROWS // STEP, step, 0)
        for dest, send, recv in ((right, send_r, recv_l), (left, send_l, recv_r)):
            copy = pltpu.make_async_remote_copy(
                src_ref=where_at(c, me), dst_ref=where_at(c, me),
                send_sem=send.at[c], recv_sem=recv.at[c],
                device_id=(bank, dest), device_id_type=MESH,
            )
            copy.start()
            sent.append(copy)

    for copy in sent0:
        copy.wait_recv()
    scale[0, :, pl.ds(0, WIDTH)] = jnp.sqrt(((sums0[0] + sums0[1]) + sums0[2]) + sums0[3])
    normalised(0)
    for copy in sent1:
        copy.wait_recv()
    total = jnp.sqrt(((sums1[0] + sums1[1]) + sums1[2]) + sums1[3])
    scale[0, :, pl.ds(WIDTH, COLS - WIDTH)] = total[:, : COLS - WIDTH]
    scale[1, :, :] = total[:, COLS - WIDTH :]
    for c in range(1, CHUNKS):
        normalised(c)
    for c in range(CHUNKS):
        write(c, me, put.at[0, c])
    for m, o in enumerate((o_sgate, o_sup)):
        copy = pltpu.make_async_copy(scale.at[m], o, small.at[m])
        copy.start()
        writes.append(copy)

    for copy in sent_x:
        copy.wait_recv()
    for k in range(4):
        bank_r[bank, pl.ds(4 * k, 4), :] = xr[k]

    def push(first, count, dest, sems, k):
        block = bank_r.at[pl.ds(first, count)]
        copy = pltpu.make_async_remote_copy(
            src_ref=block, dst_ref=block, send_sem=sems.at[0, k], recv_sem=sems.at[1, k],
            device_id=(dest, me), device_id_type=MESH,
        )
        copy.start()
        sent.append(copy)
        return copy

    push(bank, 1, twin, rc, 0).wait_recv()
    pair = at_bank(zz, yy, 0)
    a = push(pair, 2, y_up, ry, 0)
    b = push(pair, 2, y_down, ry, 1)
    a.wait_recv()
    d = push(at_bank(zz, lax.rem(yy + 3, 4), 0), 2, y_up, ry, 2)
    b.wait_recv()
    d.wait_recv()
    ups = [push(zz * 8, 8, z_up, rz, 0)]
    downs = [push(zz * 8, 8, z_down, rz, 4)]
    for k in range(1, 4):
        ups[-1].wait_recv()
        ups.append(push(lax.rem(zz + 8 - k, 8) * 8, 8, z_up, rz, k))
        downs[-1].wait_recv()
        if k < 3:
            downs.append(push(lax.rem(zz + k, 8) * 8, 8, z_down, rz, 4 + k))
    ups[-1].wait_recv()
    for k in range(RB):
        out_r[:, k * 128 : (k + 1) * 128] = bank_r[:, k, :].astype(jnp.bfloat16)
    copy = pltpu.make_async_copy(out_r, o_router, small.at[2])
    copy.start()
    writes.append(copy)

    def forward(c, owner, dest):
        copy = pltpu.make_async_remote_copy(
            src_ref=where_at(c, owner), dst_ref=where_at(c, owner),
            send_sem=fsend.at[c], recv_sem=frecv.at[c],
            device_id=(bank, dest), device_id_type=MESH,
        )
        copy.start()
        return copy

    passed = []
    for c in range(CHUNKS):
        sent[2 * c].wait_recv()
        if c < PER:
            passed.append(forward(c, left, right))
        sent[2 * c + 1].wait_recv()
        if c >= PER:
            passed.append(forward(c, right, left))
        write(c, left, put.at[1, c])
        write(c, right, put.at[2, c])
    for c in range(PER):
        passed[c].wait_recv()
        write(c, across, put.at[3, c])
        passed[c + PER].wait_recv()
        write(c + PER, across, put.at[3, c + PER])

    for copy in sent0 + sent1 + sent_x + sent + passed:
        copy.wait_send()
    for copy in writes:
        copy.wait()


def local(w_gate, avg_gate, w_up, avg_up, mix_share, router_weight, router_gain):
    dma = pltpu.SemaphoreType.DMA
    f32, bf16 = jnp.float32, jnp.bfloat16
    anywhere = pl.BlockSpec(memory_space=pl.ANY)
    outs = pl.pallas_call(
        kernel,
        out_shape=(
            jax.ShapeDtypeStruct((4 * ROWS, COLS), bf16),
            jax.ShapeDtypeStruct((4 * ROWS, COLS), bf16),
            jax.ShapeDtypeStruct((1, COLS), f32),
            jax.ShapeDtypeStruct((1, COLS), f32),
            jax.ShapeDtypeStruct((64, RB * 128), bf16),
        ),
        in_specs=[anywhere] * 7,
        out_specs=[anywhere] * 5,
        scratch_shapes=[
            pltpu.VMEM((CHUNKS, ROWS, WIDTH), f32),
            pltpu.VMEM((CHUNKS, ROWS, WIDTH), f32),
            dma((CHUNKS,)),
            dma((CHUNKS,)),
            pltpu.SMEM((1,), f32),
            dma(()),
            pltpu.VMEM((1, ROWS), f32),
            pltpu.VMEM((1, ROWS), f32),
            dma(()),
            dma(()),
            pltpu.VMEM((4, 1, WIDTH), f32),
            pltpu.VMEM((4, 1, (CHUNKS - 1) * WIDTH), f32),
            pltpu.VMEM((2, 1, COLS), f32),
            dma((2, 3)),
            dma((2, 3)),
            pltpu.VMEM((2, 4 * ROWS, COLS), bf16),
            dma((CHUNKS,)),
            dma((CHUNKS,)),
            dma((CHUNKS,)),
            dma((CHUNKS,)),
            dma((CHUNKS,)),
            dma((CHUNKS,)),
            dma((4, CHUNKS)),
            dma((1,)),
            pltpu.VMEM((4, 4, 128), f32),
            pltpu.VMEM((64, RB, 128), f32),
            pltpu.VMEM((64, RB * 128), bf16),
            dma((3,)),
            dma((3,)),
            dma((2, 1)),
            dma((2, 3)),
            dma((2, 7)),
            dma((3,)),
        ],
        compiler_params=pltpu.CompilerParams(
            collective_id=0, has_side_effects=True, vmem_limit_bytes=67043328
        ),
        name="mean_and_gather",
    )(
        w_gate[0], avg_gate[0], w_up[0], avg_up[0], mix_share,
        router_weight.T, router_gain[None, :],
    )
    gate, up, sgate, sup, router = outs
    return gate[None], up[None], sgate, sup, router.T


def solution(mesh):
    placed = (
        P("bank", "zero", None),
        P("bank", "zero", None),
        P("bank", "zero", None),
        P("bank", "zero", None),
        P("bank"),
        P("zero", "bank"),
        P("zero"),
    )
    return jax.shard_map(
        local,
        mesh=mesh,
        in_specs=placed,
        out_specs=(
            P("bank", None, None),
            P("bank", None, None),
            P("bank", None),
            P("bank", None),
            P(),
        ),
        check_vma=False,
    )
```

```python
import jax
import jax.numpy as jnp
from jax import lax
from jax.experimental import pallas as pl
from jax.experimental.pallas import tpu as pltpu
from jax.sharding import PartitionSpec as P

MESH = pl.DeviceIdType.MESH
ROWS = 512
COLS = 1024
WIDTH = 256
PER = COLS // WIDTH
CHUNKS = 2 * PER
STEP = 64
RB = 16


def kernel(
    w_gate, avg_gate, w_up, avg_up, mix, router_w, router_g,
    o_gate, o_up, o_sgate, o_sup, o_router,
    wide, other, wide_sem, other_sem, mix_s, mix_sem, rw, rg, rw_sem, rg_sem,
    sums0, sums1, sums_send, sums_recv,
    send_r, send_l, recv_l, recv_r, fsend, frecv,
    xr, bank_r, rx_send, rx_recv, rc, ry, rz,
):
    bank = lax.axis_index("bank")
    me = lax.axis_index("zero")
    right, left, across = lax.rem(me + 1, 4), lax.rem(me + 3, 4), lax.rem(me + 2, 4)
    core = lax.rem(bank, 2)
    yy = lax.rem(bank // 2, 4)
    zz = bank // 8

    def at_bank(z, y, c):
        return (z * 4 + y) * 2 + c

    twin = at_bank(zz, yy, 1 - core)
    y_up, y_down = at_bank(zz, lax.rem(yy + 1, 4), core), at_bank(zz, lax.rem(yy + 3, 4), core)
    z_up, z_down = at_bank(lax.rem(zz + 1, 8), yy, core), at_bank(lax.rem(zz + 7, 8), yy, core)

    outs, scales = (o_gate, o_up), (o_sgate, o_sup)
    w_in, a_in = (w_gate, w_up), (avg_gate, avg_up)

    mix_copy = pltpu.make_async_copy(mix, mix_s, mix_sem)
    mix_copy.start()
    loads = []
    for c in range(CHUNKS):
        m, cols = c // PER, pl.ds((c % PER) * WIDTH, WIDTH)
        first = pltpu.make_async_copy(w_in[m].at[:, cols], wide.at[c], wide_sem.at[c])
        second = pltpu.make_async_copy(a_in[m].at[:, cols], other.at[c], other_sem.at[c])
        first.start()
        second.start()
        loads.append((first, second))
    load_rw = pltpu.make_async_copy(router_w, rw, rw_sem)
    load_rg = pltpu.make_async_copy(router_g, rg, rg_sem)
    load_rw.start()
    load_rg.start()

    barrier = pltpu.get_barrier_semaphore()
    for where in (
        (bank, right), (bank, left), (bank, across),
        (twin, me), (y_up, me), (y_down, me), (z_up, me), (z_down, me),
    ):
        pl.semaphore_signal(barrier, inc=1, device_id=where, device_id_type=MESH)

    mix_copy.wait()
    share = mix_s[...]
    rest = 1.0 - share

    def mixed(c):
        loads[c][0].wait()
        loads[c][1].wait()

        def step(i, acc):
            rows = pl.ds(i * STEP, STEP)
            fresh = share * wide[c, rows, :] + rest * other[c, rows, :]
            wide[c, rows, :] = fresh
            return acc + jnp.sum((fresh * fresh).reshape(STEP // 8, 8, WIDTH), axis=0)

        acc = lax.fori_loop(0, ROWS // STEP, step, jnp.zeros((8, WIDTH), jnp.float32))
        return jnp.sum(acc, axis=0, keepdims=True)

    peers = (right, left, across)

    def share_sums(buf, g):
        copies = []
        for k, peer in enumerate(peers):
            copy = pltpu.make_async_remote_copy(
                src_ref=buf.at[me], dst_ref=buf.at[me],
                send_sem=sums_send.at[g, k], recv_sem=sums_recv.at[g, k],
                device_id=(bank, peer), device_id_type=MESH,
            )
            copy.start()
            copies.append(copy)
        return copies

    sums0[me] = mixed(0)
    pl.semaphore_wait(barrier, 8)
    sent0 = share_sums(sums0, 0)

    load_rw.wait()
    load_rg.wait()
    prod = rw[...] * rg[...]
    for k in range(4):
        xr[me, pl.ds(k, 1), :] = prod[:, k * 128 : (k + 1) * 128]
    sent_x = []
    for k, peer in enumerate(peers):
        copy = pltpu.make_async_remote_copy(
            src_ref=xr.at[me], dst_ref=xr.at[me],
            send_sem=rx_send.at[k], recv_sem=rx_recv.at[k],
            device_id=(bank, peer), device_id_type=MESH,
        )
        copy.start()
        sent_x.append(copy)

    for c in range(1, CHUNKS):
        sums1[me, :, pl.ds((c - 1) * WIDTH, WIDTH)] = mixed(c)
    sent1 = share_sums(sums1, 1)

    def where_at(c, owner):
        return outs[c // PER].at[pl.ds(owner * ROWS, ROWS), pl.ds((c % PER) * WIDTH, WIDTH)]

    sent = []

    def normalised(c):
        s = scales[c // PER][:, pl.ds((c % PER) * WIDTH, WIDTH)]
        inverse = 1.0 / s

        def step(i, carry):
            rows = pl.ds(i * STEP, STEP)
            outs[c // PER][
                pl.ds(pl.multiple_of(me * ROWS + i * STEP, STEP), STEP),
                pl.ds((c % PER) * WIDTH, WIDTH),
            ] = (wide[c, rows, :] * inverse).astype(jnp.bfloat16)
            return carry

        lax.fori_loop(0, ROWS // STEP, step, 0)
        for dest, send, recv in ((right, send_r, recv_l), (left, send_l, recv_r)):
            copy = pltpu.make_async_remote_copy(
                src_ref=where_at(c, me), dst_ref=where_at(c, me),
                send_sem=send.at[c], recv_sem=recv.at[c],
                device_id=(bank, dest), device_id_type=MESH,
            )
            copy.start()
            sent.append(copy)

    for copy in sent0:
        copy.wait_recv()
    o_sgate[:, pl.ds(0, WIDTH)] = jnp.sqrt(((sums0[0] + sums0[1]) + sums0[2]) + sums0[3])
    normalised(0)
    for copy in sent1:
        copy.wait_recv()
    total = jnp.sqrt(((sums1[0] + sums1[1]) + sums1[2]) + sums1[3])
    o_sgate[:, pl.ds(WIDTH, COLS - WIDTH)] = total[:, : COLS - WIDTH]
    o_sup[...] = total[:, COLS - WIDTH :]
    for c in range(1, CHUNKS):
        normalised(c)

    for copy in sent_x:
        copy.wait_recv()
    for k in range(4):
        bank_r[bank, pl.ds(4 * k, 4), :] = xr[k]

    def push(first, count, dest, sems, k):
        block = bank_r.at[pl.ds(first, count)]
        copy = pltpu.make_async_remote_copy(
            src_ref=block, dst_ref=block, send_sem=sems.at[0, k], recv_sem=sems.at[1, k],
            device_id=(dest, me), device_id_type=MESH,
        )
        copy.start()
        sent.append(copy)
        return copy

    push(bank, 1, twin, rc, 0).wait_recv()
    pair = at_bank(zz, yy, 0)
    a = push(pair, 2, y_up, ry, 0)
    b = push(pair, 2, y_down, ry, 1)
    a.wait_recv()
    d = push(at_bank(zz, lax.rem(yy + 3, 4), 0), 2, y_up, ry, 2)
    b.wait_recv()
    d.wait_recv()
    ups = [push(zz * 8, 8, z_up, rz, 0)]
    downs = [push(zz * 8, 8, z_down, rz, 4)]
    for k in range(1, 4):
        ups[-1].wait_recv()
        ups.append(push(lax.rem(zz + 8 - k, 8) * 8, 8, z_up, rz, k))
        downs[-1].wait_recv()
        if k < 3:
            downs.append(push(lax.rem(zz + k, 8) * 8, 8, z_down, rz, 4 + k))
    ups[-1].wait_recv()
    for k in range(RB):
        o_router[:, k * 128 : (k + 1) * 128] = bank_r[:, k, :].astype(jnp.bfloat16)

    def forward(c, owner, dest):
        copy = pltpu.make_async_remote_copy(
            src_ref=where_at(c, owner), dst_ref=where_at(c, owner),
            send_sem=fsend.at[c], recv_sem=frecv.at[c],
            device_id=(bank, dest), device_id_type=MESH,
        )
        copy.start()
        return copy

    passed = []
    for c in range(CHUNKS):
        sent[2 * c].wait_recv()
        if c < PER:
            passed.append(forward(c, left, right))
        sent[2 * c + 1].wait_recv()
        if c >= PER:
            passed.append(forward(c, right, left))
    for c in range(PER):
        passed[c].wait_recv()
        passed[c + PER].wait_recv()

    for copy in sent0 + sent1 + sent_x + sent + passed:
        copy.wait_send()


def put_out(gate, up, sgate, sup, router, o_gate, o_up, o_sgate, o_sup, o_router, sem):
    copies = []
    for i, (a, b) in enumerate(((gate, o_gate), (up, o_up))):
        for k in range(4):
            rows = pl.ds(k * ROWS, ROWS)
            copies.append(pltpu.make_async_copy(a.at[rows], b.at[rows], sem.at[4 * i + k]))
    copies.append(pltpu.make_async_copy(router, o_router, sem.at[8]))
    copies.append(pltpu.make_async_copy(sgate, o_sgate, sem.at[9]))
    copies.append(pltpu.make_async_copy(sup, o_sup, sem.at[10]))
    for copy in copies:
        copy.start()
    for copy in copies:
        copy.wait()


def local(w_gate, avg_gate, w_up, avg_up, mix_share, router_weight, router_gain):
    dma = pltpu.SemaphoreType.DMA
    f32, bf16 = jnp.float32, jnp.bfloat16
    anywhere = pl.BlockSpec(memory_space=pl.ANY)
    shapes = (
            jax.ShapeDtypeStruct((4 * ROWS, COLS), bf16),
            jax.ShapeDtypeStruct((4 * ROWS, COLS), bf16),
            jax.ShapeDtypeStruct((1, COLS), f32),
            jax.ShapeDtypeStruct((1, COLS), f32),
            jax.ShapeDtypeStruct((64, RB * 128), bf16),
    )
    held = (
            pltpu.VMEM((4 * ROWS, COLS), bf16),
            pltpu.VMEM((4 * ROWS, COLS), bf16),
            pltpu.VMEM((1, COLS), f32),
            pltpu.VMEM((1, COLS), f32),
            pltpu.VMEM((64, RB * 128), bf16),
    )
    outs = pl.pallas_call(
        kernel,
        out_shape=held,
        in_specs=[anywhere] * 7,
        out_specs=[pl.BlockSpec(memory_space=pltpu.VMEM)] * 5,
        scratch_shapes=[
            pltpu.VMEM((CHUNKS, ROWS, WIDTH), f32),
            pltpu.VMEM((CHUNKS, ROWS, WIDTH), f32),
            dma((CHUNKS,)),
            dma((CHUNKS,)),
            pltpu.VMEM((1, 1), f32),
            dma(()),
            pltpu.VMEM((1, ROWS), f32),
            pltpu.VMEM((1, ROWS), f32),
            dma(()),
            dma(()),
            pltpu.VMEM((4, 1, WIDTH), f32),
            pltpu.VMEM((4, 1, (CHUNKS - 1) * WIDTH), f32),
            dma((2, 3)),
            dma((2, 3)),
            dma((CHUNKS,)),
            dma((CHUNKS,)),
            dma((CHUNKS,)),
            dma((CHUNKS,)),
            dma((CHUNKS,)),
            dma((CHUNKS,)),
            pltpu.VMEM((4, 4, 128), f32),
            pltpu.VMEM((64, RB, 128), f32),
            dma((3,)),
            dma((3,)),
            dma((2, 1)),
            dma((2, 3)),
            dma((2, 7)),
        ],
        compiler_params=pltpu.CompilerParams(
            collective_id=0, has_side_effects=True, vmem_limit_bytes=53 * 1024 * 1024
        ),
        name="mean_and_gather",
    )(
        w_gate[0], avg_gate[0], w_up[0], avg_up[0], mix_share[:, None],
        router_weight.T, router_gain[None, :],
    )
    outs = pl.pallas_call(
        put_out,
        out_shape=shapes,
        in_specs=[pl.BlockSpec(memory_space=pltpu.VMEM)] * 5,
        out_specs=[anywhere] * 5,
        scratch_shapes=[dma((11,))],
        compiler_params=pltpu.CompilerParams(vmem_limit_bytes=1024 * 1024),
        name="put_out",
    )(*outs)
    gate, up, sgate, sup, router = outs
    return gate[None], up[None], sgate, sup, router.T


def solution(mesh):
    placed = (
        P("bank", "zero", None),
        P("bank", "zero", None),
        P("bank", "zero", None),
        P("bank", "zero", None),
        P("bank"),
        P("zero", "bank"),
        P("zero"),
    )
    return jax.shard_map(
        local,
        mesh=mesh,
        in_specs=placed,
        out_specs=(
            P("bank", None, None),
            P("bank", None, None),
            P("bank", None),
            P("bank", None),
            P(),
        ),
        check_vma=False,
    )
```

```python
import jax
import jax.numpy as jnp
from jax import lax
from jax.experimental import pallas as pl
from jax.experimental.pallas import tpu as pltpu
from jax.sharding import PartitionSpec as P

MESH = pl.DeviceIdType.MESH
ROWS = 512
COLS = 1024
WIDTH = 256
PER = COLS // WIDTH
CHUNKS = 2 * PER
STEP = 64
RB = 16
EARLY = 2


def kernel(
    w_gate, avg_gate, w_up, avg_up, mix, router_w, router_g,
    o_gate, o_up, o_sgate, o_sup, o_router,
    wide, other, wide_sem, other_sem, rw, rg, rw_sem, rg_sem,
    sums0, sums1, sums_send, sums_recv,
    send_r, send_l, recv_l, recv_r, fsend, frecv,
    xr, bank_r, rx_send, rx_recv, rc, ry, rz, joined, ready, go,
):
    bank = lax.axis_index("bank")
    me = lax.axis_index("zero")
    right, left, across = lax.rem(me + 1, 4), lax.rem(me + 3, 4), lax.rem(me + 2, 4)
    core = lax.rem(bank, 2)
    yy = lax.rem(bank // 2, 4)
    zz = bank // 8

    def at_bank(z, y, c):
        return (z * 4 + y) * 2 + c

    twin = at_bank(zz, yy, 1 - core)
    y_up, y_down = at_bank(zz, lax.rem(yy + 1, 4), core), at_bank(zz, lax.rem(yy + 3, 4), core)
    z_up, z_down = at_bank(lax.rem(zz + 1, 8), yy, core), at_bank(lax.rem(zz + 7, 8), yy, core)
    outs, scales = (o_gate, o_up), (o_sgate, o_sup)
    w_in, a_in = (w_gate, w_up), (avg_gate, avg_up)

    loads = []
    for c in range(CHUNKS):
        m, cols = c // PER, pl.ds((c % PER) * WIDTH, WIDTH)
        loads.append((
            pltpu.make_async_copy(w_in[m].at[:, cols], wide.at[c], wide_sem.at[c]),
            pltpu.make_async_copy(a_in[m].at[:, cols], other.at[c], other_sem.at[c]),
        ))
    load_rw = pltpu.make_async_copy(router_w, rw, rw_sem)
    load_rg = pltpu.make_async_copy(router_g, rg, rg_sem)

    def start_loads(first, last):
        for c in range(first, last):
            for copy in loads[c]:
                copy.start()

    start_loads(0, EARLY)

    barrier = pltpu.get_barrier_semaphore()
    lead = me == 0
    for step in range(1, 4):
        @pl.when(me + step < 4)
        def _():
            pl.semaphore_signal(barrier, inc=1, device_id=(bank, lax.rem(me + step, 4)), device_id_type=MESH)

    beside = (twin, y_up, y_down, z_up, z_down)

    @pl.when(lead)
    def _():
        for where in beside:
            pl.semaphore_signal(barrier, inc=1, device_id=(where, 0), device_id_type=MESH)

    for i in range(1, 4):
        @pl.when(me == i)
        def _():
            pl.semaphore_wait(barrier, i)
            for j in range(i):
                pl.semaphore_signal(joined, inc=1, device_id=(bank, j), device_id_type=MESH)

    share = jnp.full((8, WIDTH), mix[0], jnp.float32)
    rest = 1.0 - share

    def mixed(c):
        loads[c][0].wait()
        loads[c][1].wait()

        def step(i, acc):
            for k in range(STEP // 8):
                rows = pl.ds(pl.multiple_of(i * STEP + 8 * k, 8), 8)
                fresh = share * wide[c, rows, :] + rest * other[c, rows, :]
                wide[c, rows, :] = fresh
                acc[k % 4] += fresh * fresh
            return acc

        acc = lax.fori_loop(0, ROWS // STEP, step, [jnp.zeros((8, WIDTH), jnp.float32)] * 4)
        return jnp.sum((acc[0] + acc[1]) + (acc[2] + acc[3]), axis=0, keepdims=True)

    peers = (right, left, across)

    def share_sums(buf, g):
        copies = []
        for k in (2, 0, 1):
            copy = pltpu.make_async_remote_copy(
                src_ref=buf.at[me], dst_ref=buf.at[me],
                send_sem=sums_send.at[g, k], recv_sem=sums_recv.at[g, k],
                device_id=(bank, peers[k]), device_id_type=MESH,
            )
            copy.start()
            copies.append(copy)
        return copies

    sums0[me] = mixed(0)
    start_loads(EARLY, CHUNKS)
    load_rw.start()
    load_rg.start()
    for i in range(3):
        @pl.when(me == i)
        def _():
            pl.semaphore_wait(joined, 3 - i)

    sent0 = share_sums(sums0, 0)

    for c in range(1, CHUNKS):
        sums1[me, :, pl.ds((c - 1) * WIDTH, WIDTH)] = mixed(c)
    sent1 = share_sums(sums1, 1)

    load_rw.wait()
    load_rg.wait()
    prod = rw[...] * rg[...]
    for k in range(4):
        xr[me, pl.ds(k, 1), :] = prod[:, k * 128 : (k + 1) * 128]
    sent_x = []
    for k, peer in enumerate(peers):
        copy = pltpu.make_async_remote_copy(
            src_ref=xr.at[me], dst_ref=xr.at[me],
            send_sem=rx_send.at[k], recv_sem=rx_recv.at[k],
            device_id=(bank, peer), device_id_type=MESH,
        )
        copy.start()
        sent_x.append(copy)

    def where_at(c, owner):
        return outs[c // PER].at[pl.ds(owner * ROWS, ROWS), pl.ds((c % PER) * WIDTH, WIDTH)]

    sent = []

    def normalised(c):
        s = scales[c // PER][:, pl.ds((c % PER) * WIDTH, WIDTH)]
        inverse = jnp.broadcast_to(1.0 / s, (16, WIDTH))

        def step(i, carry):
            for k in range(STEP // 16):
                outs[c // PER][
                    pl.ds(pl.multiple_of(me * ROWS + i * STEP + 16 * k, 16), 16),
                    pl.ds((c % PER) * WIDTH, WIDTH),
                ] = (wide[c, pl.ds(pl.multiple_of(i * STEP + 16 * k, 16), 16), :] * inverse).astype(jnp.bfloat16)
            return carry

        lax.fori_loop(0, ROWS // STEP, step, 0)
        for dest, send, recv in ((right, send_r, recv_l), (left, send_l, recv_r)):
            copy = pltpu.make_async_remote_copy(
                src_ref=where_at(c, me), dst_ref=where_at(c, me),
                send_sem=send.at[c], recv_sem=recv.at[c],
                device_id=(bank, dest), device_id_type=MESH,
            )
            copy.start()
            sent.append(copy)

    for copy in sent0:
        copy.wait_recv()
    o_sgate[:, pl.ds(0, WIDTH)] = jnp.sqrt(((sums0[0] + sums0[1]) + sums0[2]) + sums0[3])
    normalised(0)
    for copy in sent1:
        copy.wait_recv()
    total = jnp.sqrt(((sums1[0] + sums1[1]) + sums1[2]) + sums1[3])
    o_sgate[:, pl.ds(WIDTH, COLS - WIDTH)] = total[:, : COLS - WIDTH]
    o_sup[...] = total[:, COLS - WIDTH :]
    for c in range(1, CHUNKS):
        normalised(c)

    @pl.when(lead)
    def _():
        pl.semaphore_wait(barrier, len(beside))
        for where in beside:
            pl.semaphore_signal(ready, inc=1, device_id=(where, 0), device_id_type=MESH)
        pl.semaphore_wait(ready, len(beside))
        for j in range(1, 4):
            pl.semaphore_signal(go, inc=1, device_id=(bank, j), device_id_type=MESH)

    @pl.when(me > 0)
    def _():
        pl.semaphore_wait(go, 1)

    for copy in sent_x:
        copy.wait_recv()
    for k in range(4):
        bank_r[bank, pl.ds(4 * k, 4), :] = xr[k]

    def push(first, count, dest, sems, k):
        block = bank_r.at[pl.ds(first, count)]
        copy = pltpu.make_async_remote_copy(
            src_ref=block, dst_ref=block, send_sem=sems.at[0, k], recv_sem=sems.at[1, k],
            device_id=(dest, me), device_id_type=MESH,
        )
        copy.start()
        sent.append(copy)
        return copy

    push(bank, 1, twin, rc, 0).wait_recv()
    pair = at_bank(zz, yy, 0)
    a = push(pair, 2, y_up, ry, 0)
    b = push(pair, 2, y_down, ry, 1)
    a.wait_recv()
    d = push(at_bank(zz, lax.rem(yy + 3, 4), 0), 2, y_up, ry, 2)
    b.wait_recv()
    d.wait_recv()
    ups = [push(zz * 8, 8, z_up, rz, 0)]
    downs = [push(zz * 8, 8, z_down, rz, 4)]
    for k in range(1, 4):
        ups[-1].wait_recv()
        ups.append(push(lax.rem(zz + 8 - k, 8) * 8, 8, z_up, rz, k))
        downs[-1].wait_recv()
        if k < 3:
            downs.append(push(lax.rem(zz + k, 8) * 8, 8, z_down, rz, 4 + k))
    ups[-1].wait_recv()
    for k in range(RB):
        o_router[:, k * 128 : (k + 1) * 128] = bank_r[:, k, :].astype(jnp.bfloat16)

    def forward(c, owner, dest):
        copy = pltpu.make_async_remote_copy(
            src_ref=where_at(c, owner), dst_ref=where_at(c, owner),
            send_sem=fsend.at[c], recv_sem=frecv.at[c],
            device_id=(bank, dest), device_id_type=MESH,
        )
        copy.start()
        return copy

    passed = []
    for c in range(CHUNKS):
        sent[2 * c].wait_recv()
        if c < PER:
            passed.append(forward(c, left, right))
        sent[2 * c + 1].wait_recv()
        if c >= PER:
            passed.append(forward(c, right, left))
    for c in range(PER):
        passed[c].wait_recv()
        passed[c + PER].wait_recv()

    for copy in sent0 + sent1 + sent_x + sent + passed:
        copy.wait_send()


def put_out(gate, up, sgate, sup, router, o_gate, o_up, o_sgate, o_sup, o_router, sem):
    copies = []
    for i, (a, b) in enumerate(((gate, o_gate), (up, o_up))):
        for k in range(4):
            rows = pl.ds(k * ROWS, ROWS)
            copies.append(pltpu.make_async_copy(a.at[rows], b.at[rows], sem.at[4 * i + k]))
    copies.append(pltpu.make_async_copy(router, o_router, sem.at[8]))
    copies.append(pltpu.make_async_copy(sgate, o_sgate, sem.at[9]))
    copies.append(pltpu.make_async_copy(sup, o_sup, sem.at[10]))
    for copy in copies:
        copy.start()
    for copy in copies:
        copy.wait()


def local(w_gate, avg_gate, w_up, avg_up, mix_share, router_weight, router_gain):
    dma, regular = pltpu.SemaphoreType.DMA, pltpu.SemaphoreType.REGULAR
    f32, bf16 = jnp.float32, jnp.bfloat16
    anywhere = pl.BlockSpec(memory_space=pl.ANY)
    in_vmem = pl.BlockSpec(memory_space=pltpu.VMEM)
    results = (
        ((4 * ROWS, COLS), bf16), ((4 * ROWS, COLS), bf16),
        ((1, COLS), f32), ((1, COLS), f32), ((64, RB * 128), bf16),
    )
    held = pl.pallas_call(
        kernel,
        out_shape=tuple(pltpu.VMEM(*r) for r in results),
        in_specs=[anywhere] * 4 + [pl.BlockSpec(memory_space=pltpu.SMEM)] + [anywhere] * 2,
        out_specs=[in_vmem] * 5,
        scratch_shapes=[
            pltpu.VMEM((CHUNKS, ROWS, WIDTH), f32),
            pltpu.VMEM((CHUNKS, ROWS, WIDTH), f32),
            dma((CHUNKS,)),
            dma((CHUNKS,)),
            pltpu.VMEM((1, ROWS), f32),
            pltpu.VMEM((1, ROWS), f32),
            dma(()),
            dma(()),
            pltpu.VMEM((4, 1, WIDTH), f32),
            pltpu.VMEM((4, 1, (CHUNKS - 1) * WIDTH), f32),
            dma((2, 3)),
            dma((2, 3)),
            dma((CHUNKS,)),
            dma((CHUNKS,)),
            dma((CHUNKS,)),
            dma((CHUNKS,)),
            dma((CHUNKS,)),
            dma((CHUNKS,)),
            pltpu.VMEM((4, 4, 128), f32),
            pltpu.VMEM((64, RB, 128), f32),
            dma((3,)),
            dma((3,)),
            dma((2, 1)),
            dma((2, 3)),
            dma((2, 7)),
            regular,
            regular,
            regular,
        ],
        compiler_params=pltpu.CompilerParams(
            collective_id=0, has_side_effects=True, vmem_limit_bytes=53 * 1024 * 1024
        ),
        name="mean_and_gather",
    )(
        w_gate[0], avg_gate[0], w_up[0], avg_up[0], mix_share,
        router_weight.T, router_gain[None, :],
    )
    gate, up, sgate, sup, router = pl.pallas_call(
        put_out,
        out_shape=tuple(jax.ShapeDtypeStruct(*r) for r in results),
        in_specs=[in_vmem] * 5,
        out_specs=[anywhere] * 5,
        scratch_shapes=[dma((11,))],
        compiler_params=pltpu.CompilerParams(vmem_limit_bytes=1024 * 1024),
        name="put_out",
    )(*held)
    return gate[None], up[None], sgate, sup, router.T


def solution(mesh):
    placed = (
        P("bank", "zero", None),
        P("bank", "zero", None),
        P("bank", "zero", None),
        P("bank", "zero", None),
        P("bank"),
        P("zero", "bank"),
        P("zero"),
    )
    return jax.shard_map(
        local,
        mesh=mesh,
        in_specs=placed,
        out_specs=(
            P("bank", None, None),
            P("bank", None, None),
            P("bank", None),
            P("bank", None),
            P(),
        ),
        check_vma=False,
    )
```

```python
import jax
import jax.numpy as jnp
from jax import lax
from jax.experimental import pallas as pl
from jax.experimental.pallas import tpu as pltpu
from jax.sharding import PartitionSpec as P

MESH = pl.DeviceIdType.MESH
ROWS = 512
COLS = 1024
WIDTH = 256
HALF = WIDTH // 2
PER = COLS // WIDTH
STEP = 128
RB = 16
RAW = 320
LOADS = ((0, 0, WIDTH), (0, WIDTH, WIDTH), (0, 2 * WIDTH, 2 * WIDTH), (1, 0, 2 * WIDTH), (1, 2 * WIDTH, 2 * WIDTH))


def kernel(
    w_gate, avg_gate, w_up, avg_up, mix, router_w, router_g,
    o_gate, o_up, o_sgate, o_sup, o_router,
    wide, other, load_sem, router_in, router_sem,
    sums0, sums1, sums2, sums_send, sums_recv, raw_in, raw_send, raw_recv,
    bulk_send, gate_recv, up_recv, late_recv, pass_send, pass_recv,
    xr, bank_r, x_send, x_recv, b_send, twin_recv, y_recv, z_recv, joined, ready, go,
):
    bank = lax.axis_index("bank")
    me = lax.axis_index("zero")
    right, left, across = lax.rem(me + 1, 4), lax.rem(me + 3, 4), lax.rem(me + 2, 4)
    core = lax.rem(bank, 2)
    yy = lax.rem(bank // 2, 4)
    zz = bank // 8

    def at_bank(z, y, c):
        return (z * 4 + y) * 2 + c

    twin = at_bank(zz, yy, 1 - core)
    y_up, y_down = at_bank(zz, lax.rem(yy + 1, 4), core), at_bank(zz, lax.rem(yy + 3, 4), core)
    z_up, z_down = at_bank(lax.rem(zz + 1, 8), yy, core), at_bank(lax.rem(zz + 7, 8), yy, core)
    outs, scales = (o_gate, o_up), (o_sgate, o_sup)
    w_in, a_in = (w_gate, w_up), (avg_gate, avg_up)

    def remote(src, dst, send, recv, where, who):
        return pltpu.make_async_remote_copy(
            src_ref=src, dst_ref=dst, send_sem=send, recv_sem=recv,
            device_id=(where, who), device_id_type=MESH,
        )

    def arrived(ref, sem):
        remote(ref, ref, sem, sem, bank, right).wait_recv()

    def departed(ref, sem):
        remote(ref, ref, sem, sem, bank, right).wait_send()

    def start_load(k):
        m, first, count = LOADS[k]
        cols = pl.ds(first, count)
        pltpu.make_async_copy(w_in[m].at[:, cols], wide.at[m, :, cols], load_sem.at[k]).start()
        pltpu.make_async_copy(a_in[m].at[:, cols], other.at[m, :, cols], load_sem.at[k]).start()

    def loaded(k):
        both = pl.ds(0, 2 * LOADS[k][2])
        pltpu.make_async_copy(w_gate.at[:, both], wide.at[0, :, both], load_sem.at[k]).wait()

    start_load(0)
    start_load(1)

    barrier = pltpu.get_barrier_semaphore()
    lead = me == 0
    beside = (twin, y_up, y_down, z_up, z_down)

    def greet(where, who):
        pl.semaphore_signal(barrier, inc=1, device_id=(where, who), device_id_type=MESH)

    for step in range(1, 4):
        @pl.when(me + step < 4)
        def _():
            greet(bank, lax.rem(me + step, 4))

    @pl.when(lead)
    def _():
        for where in beside:
            greet(where, 0)

    for i in range(1, 4):
        @pl.when(me == i)
        def _():
            pl.semaphore_wait(barrier, i)
            for j in range(i):
                pl.semaphore_signal(joined, inc=1, device_id=(bank, j), device_id_type=MESH)

    share = jnp.full((8, WIDTH), mix[0], jnp.float32)
    rest = 1.0 - share

    def mixed(c):
        m, cols = c // PER, pl.ds((c % PER) * WIDTH, WIDTH)

        def step(i, acc):
            for k in range(STEP // 8):
                rows = pl.ds(pl.multiple_of(i * STEP + 8 * k, 8), 8)
                fresh = share * wide[m, rows, cols] + rest * other[m, rows, cols]
                wide[m, rows, cols] = fresh
                acc[k % 4] += fresh * fresh
            return acc

        acc = lax.fori_loop(0, ROWS // STEP, step, [jnp.zeros((8, WIDTH), jnp.float32)] * 4)
        return jnp.sum((acc[0] + acc[1]) + (acc[2] + acc[3]), axis=0, keepdims=True)

    peers = (across, right, left)

    def share_sums(buf, k):
        for peer in peers:
            remote(buf.at[me], buf.at[me], sums_send, sums_recv.at[k], bank, peer).start()

    def totals(buf, k):
        arrived(buf.at[pl.ds(0, 3)], sums_recv.at[k])
        return jnp.sqrt(((buf[0] + buf[1]) + buf[2]) + buf[3])

    loaded(0)
    sums0[me] = mixed(0)
    start_load(2)
    start_load(3)
    start_load(4)
    pltpu.make_async_copy(router_w, router_in.at[pl.ds(0, 1)], router_sem).start()
    pltpu.make_async_copy(router_g, router_in.at[pl.ds(1, 1)], router_sem).start()

    for i in range(3):
        @pl.when(me == i)
        def _():
            pl.semaphore_wait(joined, 3 - i)

    share_sums(sums0, 0)

    def send_raw(k):
        rows = pl.ds(k * RAW // 2, RAW // 2)
        for side, dest in enumerate((right, left)):
            remote(wide.at[0, rows, pl.ds(0, HALF)], raw_in.at[side, rows], raw_send, raw_recv, bank, dest).start()

    send_raw(0)
    loaded(1)
    sums1[me, :, pl.ds(0, WIDTH)] = mixed(1)
    loaded(2)
    for c in range(2, PER):
        sums1[me, :, pl.ds((c - 1) * WIDTH, WIDTH)] = mixed(c)
    share_sums(sums1, 1)
    send_raw(1)
    for k in (3, 4):
        loaded(k)
        for c in (2 * k - 2, 2 * k - 1):
            sums2[me, :, pl.ds((c - PER) * WIDTH, WIDTH)] = mixed(c)
    share_sums(sums2, 2)

    pltpu.make_async_copy(w_gate.at[pl.ds(0, 2), pl.ds(0, ROWS)], router_in, router_sem).wait()
    prod = router_in[0:1, :] * router_in[1:2, :]
    for k in range(4):
        xr[me, pl.ds(k, 1), :] = prod[:, k * 128 : (k + 1) * 128]
    for peer in peers:
        remote(xr.at[me], xr.at[me], x_send, x_recv, bank, peer).start()

    def where_at(c, owner):
        return outs[c // PER].at[pl.ds(owner * ROWS, ROWS), pl.ds((c % PER) * WIDTH, WIDTH)]

    def normalised(c):
        cols = pl.ds((c % PER) * WIDTH, WIDTH)
        inverse = jnp.broadcast_to(1.0 / scales[c // PER][:, cols], (16, WIDTH))

        def step(i, carry):
            for k in range(STEP // 16):
                rows = pl.ds(pl.multiple_of(i * STEP + 16 * k, 16), 16)
                outs[c // PER][pl.ds(pl.multiple_of(me * ROWS + i * STEP + 16 * k, 16), 16), cols] = (
                    wide[c // PER, rows, cols] * inverse
                ).astype(jnp.bfloat16)
            return carry

        lax.fori_loop(0, ROWS // STEP, step, 0)

    def send_both(block, from_left, from_right):
        remote(block, block, bulk_send, from_left, bank, right).start()
        remote(block, block, bulk_send, from_right, bank, left).start()

    o_sgate[:, pl.ds(0, WIDTH)] = totals(sums0, 0)
    normalised(0)
    send_both(o_gate.at[pl.ds(me * ROWS, ROWS), pl.ds(HALF, HALF)], gate_recv.at[0], gate_recv.at[1])
    send_both(o_gate.at[pl.ds(me * ROWS + RAW, ROWS - RAW), pl.ds(0, HALF)], gate_recv.at[0], gate_recv.at[1])
    o_sgate[:, pl.ds(WIDTH, COLS - WIDTH)] = totals(sums1, 1)
    for c in range(1, PER):
        normalised(c)
        send_both(where_at(c, me), gate_recv.at[0], gate_recv.at[1])
    o_sup[...] = totals(sums2, 2)
    for c in range(PER, 2 * PER):
        normalised(c)
        send_both(where_at(c, me), late_recv, up_recv.at[0 if c < 2 * PER - 1 else 1])

    @pl.when(lead)
    def _():
        pl.semaphore_wait(barrier, 5)
        for where in beside:
            pl.semaphore_signal(ready, inc=1, device_id=(where, 0), device_id_type=MESH)
        pl.semaphore_wait(ready, 5)
        for j in range(1, 4):
            pl.semaphore_signal(go, inc=1, device_id=(bank, j), device_id_type=MESH)

    @pl.when(jnp.logical_not(lead))
    def _():
        pl.semaphore_wait(go, 1)

    arrived(xr.at[pl.ds(0, 3)], x_recv)
    for k in range(4):
        bank_r[bank, pl.ds(4 * k, 4), :] = xr[k]

    def push(first, count, dest, recv):
        block = bank_r.at[pl.ds(first, count)]
        remote(block, block, b_send, recv, dest, me).start()

    def got(count, recv):
        arrived(bank_r.at[pl.ds(0, count)], recv)

    push(bank, 1, twin, twin_recv)
    got(1, twin_recv)
    pair = at_bank(zz, yy, 0)
    push(pair, 2, y_up, y_recv.at[0])
    push(pair, 2, y_down, y_recv.at[1])
    got(2, y_recv.at[0])
    push(at_bank(zz, lax.rem(yy + 3, 4), 0), 2, y_up, y_recv.at[1])
    got(4, y_recv.at[1])
    push(zz * 8, 8, z_up, z_recv.at[0])
    push(zz * 8, 8, z_down, z_recv.at[3])
    for k in range(1, 4):
        got(8, z_recv.at[k - 1])
        push(lax.rem(zz + 8 - k, 8) * 8, 8, z_up, z_recv.at[k if k < 3 else 5])
        if k < 3:
            got(8, z_recv.at[k + 2])
            push(lax.rem(zz + k, 8) * 8, 8, z_down, z_recv.at[k + 3])
    got(16, z_recv.at[5])
    for k in range(RB):
        o_router[:, k * 128 : (k + 1) * 128] = bank_r[:, k, :].astype(jnp.bfloat16)

    arrived(raw_in, raw_recv)
    inverse = jnp.broadcast_to(1.0 / o_sgate[:, pl.ds(0, HALF)], (16, HALF))
    for side, owner in enumerate((left, right)):
        for k in range(RAW // 16):
            o_gate[pl.ds(pl.multiple_of(owner * ROWS + 16 * k, 16), 16), pl.ds(0, HALF)] = (
                raw_in[side, pl.ds(16 * k, 16), :] * inverse
            ).astype(jnp.bfloat16)

    short = RAW * HALF // COLS
    arrived(o_gate.at[pl.ds(0, ROWS - short)], gate_recv.at[0])
    block = o_gate.at[pl.ds(left * ROWS, ROWS)]
    remote(block, block, pass_send, pass_recv.at[0], bank, right).start()
    for k, (first, count) in enumerate(((0, COLS - WIDTH), (COLS - WIDTH, WIDTH))):
        block = o_up.at[pl.ds(right * ROWS, ROWS), pl.ds(first, count)]
        arrived(block, up_recv.at[k])
        remote(block, block, pass_send, pass_recv.at[1], bank, left).start()

    arrived(o_gate.at[pl.ds(0, ROWS - short)], gate_recv.at[1])
    arrived(o_up.at[pl.ds(0, ROWS)], late_recv)
    departed(raw_in.at[0, pl.ds(0, 48)], sums_send)
    departed(raw_in, raw_send)
    departed(xr.at[pl.ds(0, 3)], x_send)
    departed(bank_r.at[pl.ds(0, 63)], b_send)
    departed(o_gate.at[pl.ds(0, 4 * ROWS - 2 * short)], bulk_send)
    arrived(o_gate.at[pl.ds(0, ROWS)], pass_recv.at[0])
    arrived(o_up.at[pl.ds(0, ROWS)], pass_recv.at[1])
    departed(o_gate.at[pl.ds(0, 2 * ROWS)], pass_send)


def put_out(gate, up, sgate, sup, router, o_gate, o_up, o_sgate, o_sup, o_router, sem):
    copies = []
    for i, (a, b) in enumerate(((gate, o_gate), (up, o_up))):
        for k in range(4):
            rows = pl.ds(k * ROWS, ROWS)
            copies.append(pltpu.make_async_copy(a.at[rows], b.at[rows], sem.at[4 * i + k]))
    copies.append(pltpu.make_async_copy(router, o_router, sem.at[8]))
    copies.append(pltpu.make_async_copy(sgate, o_sgate, sem.at[9]))
    copies.append(pltpu.make_async_copy(sup, o_sup, sem.at[10]))
    for copy in copies:
        copy.start()
    for copy in copies:
        copy.wait()


def local(w_gate, avg_gate, w_up, avg_up, mix_share, router_weight, router_gain):
    dma, regular = pltpu.SemaphoreType.DMA, pltpu.SemaphoreType.REGULAR
    f32, bf16 = jnp.float32, jnp.bfloat16
    anywhere = pl.BlockSpec(memory_space=pl.ANY)
    in_vmem = pl.BlockSpec(memory_space=pltpu.VMEM)
    results = (
        ((4 * ROWS, COLS), bf16), ((4 * ROWS, COLS), bf16),
        ((1, COLS), f32), ((1, COLS), f32), ((64, RB * 128), bf16),
    )
    held = pl.pallas_call(
        kernel,
        out_shape=tuple(pltpu.VMEM(*r) for r in results),
        in_specs=[anywhere] * 4 + [pl.BlockSpec(memory_space=pltpu.SMEM)] + [anywhere] * 2,
        out_specs=[in_vmem] * 5,
        scratch_shapes=[
            pltpu.VMEM((2, ROWS, COLS), f32),
            pltpu.VMEM((2, ROWS, COLS), f32),
            dma((len(LOADS),)),
            pltpu.VMEM((2, ROWS), f32),
            dma(()),
            pltpu.VMEM((4, 1, WIDTH), f32),
            pltpu.VMEM((4, 1, COLS - WIDTH), f32),
            pltpu.VMEM((4, 1, COLS), f32),
            dma(()),
            dma((3,)),
            pltpu.VMEM((2, RAW, HALF), f32),
            dma(()),
            dma(()),
            dma(()),
            dma((2,)),
            dma((2,)),
            dma(()),
            dma(()),
            dma((2,)),
            pltpu.VMEM((4, 4, 128), f32),
            pltpu.VMEM((64, RB, 128), f32),
            dma(()),
            dma(()),
            dma(()),
            dma(()),
            dma((2,)),
            dma((6,)),
            regular,
            regular,
            regular,
        ],
        compiler_params=pltpu.CompilerParams(
            collective_id=0, has_side_effects=True, vmem_limit_bytes=53 * 1024 * 1024
        ),
        name="mean_and_gather",
    )(
        w_gate[0], avg_gate[0], w_up[0], avg_up[0], mix_share,
        router_weight.T, router_gain[None, :],
    )
    gate, up, sgate, sup, router = pl.pallas_call(
        put_out,
        out_shape=tuple(jax.ShapeDtypeStruct(*r) for r in results),
        in_specs=[in_vmem] * 5,
        out_specs=[anywhere] * 5,
        scratch_shapes=[dma((11,))],
        compiler_params=pltpu.CompilerParams(vmem_limit_bytes=1024 * 1024),
        name="put_out",
    )(*held)
    return gate[None], up[None], sgate, sup, router.T


def solution(mesh):
    placed = (
        P("bank", "zero", None),
        P("bank", "zero", None),
        P("bank", "zero", None),
        P("bank", "zero", None),
        P("bank"),
        P("zero", "bank"),
        P("zero"),
    )
    return jax.shard_map(
        local,
        mesh=mesh,
        in_specs=placed,
        out_specs=(
            P("bank", None, None),
            P("bank", None, None),
            P("bank", None),
            P("bank", None),
            P(),
        ),
        check_vma=False,
    )
```

```python
import jax
import jax.numpy as jnp
from jax import lax
from jax.experimental import pallas as pl
from jax.experimental.pallas import tpu as pltpu
from jax.sharding import PartitionSpec as P

MESH = pl.DeviceIdType.MESH
ROWS = 512
COLS = 1024
WIDTH = 256
HALF = WIDTH // 2
PER = COLS // WIDTH
STEP = 128
RB = 16
RAW = 320
FIRST = (768, 128)
REST = COLS - min(FIRST)
LOADS = ((0, 0, WIDTH), (0, WIDTH, WIDTH), (0, 2 * WIDTH, 2 * WIDTH), (1, 0, 2 * WIDTH), (1, 2 * WIDTH, 2 * WIDTH))


def kernel(
    w_gate, avg_gate, w_up, avg_up, mix, router_w, router_g,
    o_gate, o_up, o_sgate, o_sup, o_router,
    wide, other, load_sem, router_in, router_sem,
    sums0, sums1, sums2, sums_send, sums_recv, raw_in, raw_send, raw_recv,
    bulk_send, gate_recv, up_recv, late_recv, pass_send, pass_recv,
    xr, bank_r, x_send, x_recv, b_send, twin_recv, y_recv, z_recv, joined, ready, go,
):
    bank = lax.axis_index("bank")
    me = lax.axis_index("zero")
    right, left, across = lax.rem(me + 1, 4), lax.rem(me + 3, 4), lax.rem(me + 2, 4)
    core = lax.rem(bank, 2)
    yy = lax.rem(bank // 2, 4)
    zz = bank // 8

    def at_bank(z, y, c):
        return (z * 4 + y) * 2 + c

    twin = at_bank(zz, yy, 1 - core)
    y_up, y_down = at_bank(zz, lax.rem(yy + 1, 4), core), at_bank(zz, lax.rem(yy + 3, 4), core)
    z_up, z_down = at_bank(lax.rem(zz + 1, 8), yy, core), at_bank(lax.rem(zz + 7, 8), yy, core)
    outs, scales = (o_gate, o_up), (o_sgate, o_sup)
    w_in, a_in = (w_gate, w_up), (avg_gate, avg_up)

    def remote(src, dst, send, recv, where, who):
        return pltpu.make_async_remote_copy(
            src_ref=src, dst_ref=dst, send_sem=send, recv_sem=recv,
            device_id=(where, who), device_id_type=MESH,
        )

    def arrived(ref, sem):
        remote(ref, ref, sem, sem, bank, right).wait_recv()

    def departed(ref, sem):
        remote(ref, ref, sem, sem, bank, right).wait_send()

    def start_load(k):
        m, first, count = LOADS[k]
        cols = pl.ds(first, count)
        pltpu.make_async_copy(w_in[m].at[:, cols], wide.at[m, :, cols], load_sem.at[k]).start()
        pltpu.make_async_copy(a_in[m].at[:, cols], other.at[m, :, cols], load_sem.at[k]).start()

    def loaded(k):
        both = pl.ds(0, 2 * LOADS[k][2])
        pltpu.make_async_copy(w_gate.at[:, both], wide.at[0, :, both], load_sem.at[k]).wait()

    start_load(0)
    start_load(1)

    barrier = pltpu.get_barrier_semaphore()
    lead = jnp.logical_and(core == 1, me == 0)
    beside = (y_up, y_down, z_up, z_down)

    def greet(where, who):
        pl.semaphore_signal(barrier, inc=1, device_id=(where, who), device_id_type=MESH)

    @pl.when(core == 0)
    def _():
        for peer in (across, right, left):
            greet(bank, peer)

    for step in range(1, 4):
        @pl.when(jnp.logical_and(core == 1, me + step < 4))
        def _():
            greet(bank, lax.rem(me + step, 4))

    @pl.when(lead)
    def _():
        for where in beside:
            greet(where, 0)

    for i in range(1, 4):
        @pl.when(jnp.logical_and(core == 1, me == i))
        def _():
            pl.semaphore_wait(barrier, i)
            for j in range(i):
                pl.semaphore_signal(joined, inc=1, device_id=(bank, j), device_id_type=MESH)

    share = jnp.full((8, WIDTH), mix[0], jnp.float32)
    rest = 1.0 - share

    def mixed(c):
        m, cols = c // PER, pl.ds((c % PER) * WIDTH, WIDTH)

        def step(i, acc):
            for k in range(STEP // 8):
                rows = pl.ds(pl.multiple_of(i * STEP + 8 * k, 8), 8)
                fresh = share * wide[m, rows, cols] + rest * other[m, rows, cols]
                wide[m, rows, cols] = fresh
                acc[k % 4] += fresh * fresh
            return acc

        acc = lax.fori_loop(0, ROWS // STEP, step, [jnp.zeros((8, WIDTH), jnp.float32)] * 4)
        return jnp.sum((acc[0] + acc[1]) + (acc[2] + acc[3]), axis=0, keepdims=True)

    peers = (across, right, left)

    def share_sums(buf, k):
        for peer in peers:
            remote(buf.at[me], buf.at[me], sums_send, sums_recv.at[k], bank, peer).start()

    def totals(buf, k):
        arrived(buf.at[pl.ds(0, 3)], sums_recv.at[k])
        return jnp.sqrt(((buf[0] + buf[1]) + buf[2]) + buf[3])

    loaded(0)
    sums0[me] = mixed(0)
    start_load(2)
    start_load(3)
    start_load(4)
    pltpu.make_async_copy(router_w, router_in.at[pl.ds(0, 1)], router_sem).start()
    pltpu.make_async_copy(router_g, router_in.at[pl.ds(1, 1)], router_sem).start()

    @pl.when(core == 0)
    def _():
        pl.semaphore_wait(barrier, 3)

    for i in range(3):
        @pl.when(jnp.logical_and(core == 1, me == i))
        def _():
            pl.semaphore_wait(joined, 3 - i)

    share_sums(sums0, 0)

    def send_raw(k):
        rows = pl.ds(k * RAW // 2, RAW // 2)
        for side, dest in enumerate((right, left)):
            remote(wide.at[0, rows, pl.ds(0, HALF)], raw_in.at[side, rows], raw_send, raw_recv, bank, dest).start()

    send_raw(0)
    loaded(1)
    sums1[me, :, pl.ds(0, WIDTH)] = mixed(1)
    loaded(2)
    for c in range(2, PER):
        sums1[me, :, pl.ds((c - 1) * WIDTH, WIDTH)] = mixed(c)
    share_sums(sums1, 1)
    send_raw(1)
    for k in (3, 4):
        loaded(k)
        for c in (2 * k - 2, 2 * k - 1):
            sums2[me, :, pl.ds((c - PER) * WIDTH, WIDTH)] = mixed(c)
    share_sums(sums2, 2)

    pltpu.make_async_copy(w_gate.at[pl.ds(0, 2), pl.ds(0, ROWS)], router_in, router_sem).wait()
    prod = router_in[0:1, :] * router_in[1:2, :]
    for k in range(4):
        xr[me, pl.ds(k, 1), :] = prod[:, k * 128 : (k + 1) * 128]
    for peer in peers:
        remote(xr.at[me], xr.at[me], x_send, x_recv, bank, peer).start()

    def where_at(c, owner):
        return outs[c // PER].at[pl.ds(owner * ROWS, ROWS), pl.ds((c % PER) * WIDTH, WIDTH)]

    def normalised(c):
        cols = pl.ds((c % PER) * WIDTH, WIDTH)
        inverse = jnp.broadcast_to(1.0 / scales[c // PER][:, cols], (16, WIDTH))

        def step(i, carry):
            for k in range(STEP // 16):
                rows = pl.ds(pl.multiple_of(i * STEP + 16 * k, 16), 16)
                outs[c // PER][pl.ds(pl.multiple_of(me * ROWS + i * STEP + 16 * k, 16), 16), cols] = (
                    wide[c // PER, rows, cols] * inverse
                ).astype(jnp.bfloat16)
            return carry

        lax.fori_loop(0, ROWS // STEP, step, 0)

    def send_both(block, from_left, from_right):
        remote(block, block, bulk_send, from_left, bank, right).start()
        remote(block, block, bulk_send, from_right, bank, left).start()

    o_sgate[:, pl.ds(0, WIDTH)] = totals(sums0, 0)
    normalised(0)
    send_both(o_gate.at[pl.ds(me * ROWS, ROWS), pl.ds(HALF, HALF)], gate_recv.at[0], gate_recv.at[1])
    send_both(o_gate.at[pl.ds(me * ROWS + RAW, ROWS - RAW), pl.ds(0, HALF)], gate_recv.at[0], gate_recv.at[1])
    o_sgate[:, pl.ds(WIDTH, COLS - WIDTH)] = totals(sums1, 1)
    for c in range(1, PER):
        normalised(c)
        send_both(where_at(c, me), gate_recv.at[0], gate_recv.at[1])
    o_sup[...] = totals(sums2, 2)
    for c in range(PER, 2 * PER):
        normalised(c)
        send_both(where_at(c, me), late_recv, up_recv.at[0 if c < 2 * PER - 1 else 1])

    @pl.when(jnp.logical_and(core == 0, me == 0))
    def _():
        greet(twin, 0)

    @pl.when(lead)
    def _():
        pl.semaphore_wait(barrier, 5)
        for where in beside:
            pl.semaphore_signal(ready, inc=1, device_id=(where, 0), device_id_type=MESH)
        pl.semaphore_wait(ready, 4)
        for j in range(1, 4):
            pl.semaphore_signal(go, inc=1, device_id=(bank, j), device_id_type=MESH)
        for j in range(4):
            pl.semaphore_signal(go, inc=1, device_id=(twin, j), device_id_type=MESH)

    @pl.when(jnp.logical_not(lead))
    def _():
        pl.semaphore_wait(go, 1)

    arrived(xr.at[pl.ds(0, 3)], x_recv)
    for k in range(4):
        bank_r[bank, pl.ds(4 * k, 4), :] = xr[k]

    def push(first, count, dest, recv):
        block = bank_r.at[pl.ds(first, count)]
        remote(block, block, b_send, recv, dest, me).start()

    def got(count, recv):
        arrived(bank_r.at[pl.ds(0, count)], recv)

    push(bank, 1, twin, twin_recv)
    got(1, twin_recv)
    pair = at_bank(zz, yy, 0)
    push(pair, 2, y_up, y_recv.at[0])
    push(pair, 2, y_down, y_recv.at[1])
    got(2, y_recv.at[0])
    push(at_bank(zz, lax.rem(yy + 3, 4), 0), 2, y_up, y_recv.at[1])
    got(4, y_recv.at[1])
    push(zz * 8, 8, z_up, z_recv.at[0])
    push(zz * 8, 8, z_down, z_recv.at[3])
    for k in range(1, 4):
        got(8, z_recv.at[k - 1])
        push(lax.rem(zz + 8 - k, 8) * 8, 8, z_up, z_recv.at[k if k < 3 else 5])
        if k < 3:
            got(8, z_recv.at[k + 2])
            push(lax.rem(zz + k, 8) * 8, 8, z_down, z_recv.at[k + 3])
    got(16, z_recv.at[5])
    for k in range(RB):
        o_router[:, k * 128 : (k + 1) * 128] = bank_r[:, k, :].astype(jnp.bfloat16)

    arrived(raw_in, raw_recv)
    inverse = jnp.broadcast_to(1.0 / o_sgate[:, pl.ds(0, HALF)], (16, HALF))
    for side, owner in enumerate((left, right)):
        for k in range(RAW // 16):
            o_gate[pl.ds(pl.multiple_of(owner * ROWS + 16 * k, 16), 16), pl.ds(0, HALF)] = (
                raw_in[side, pl.ds(16 * k, 16), :] * inverse
            ).astype(jnp.bfloat16)

    short = RAW * HALF // COLS
    arrived(o_gate.at[pl.ds(0, ROWS - short)], gate_recv.at[0])
    for which, width in enumerate(FIRST):
        @pl.when(core == which)
        def _():
            block = o_gate.at[pl.ds(left * ROWS, ROWS), pl.ds(0, width)]
            remote(block, block, pass_send, pass_recv.at[0], bank, right).start()
            for k, (first, end) in enumerate(((0, COLS - WIDTH), (COLS - WIDTH, COLS))):
                arrived(o_up.at[pl.ds(0, ROWS), pl.ds(first, end - first)], up_recv.at[k])
                if first < width:
                    block = o_up.at[pl.ds(right * ROWS, ROWS), pl.ds(first, min(end, width) - first)]
                    remote(block, block, pass_send, pass_recv.at[1], bank, left).start()

    arrived(o_gate.at[pl.ds(0, ROWS - short)], gate_recv.at[1])
    arrived(o_up.at[pl.ds(0, ROWS)], late_recv)
    departed(raw_in.at[0, pl.ds(0, 48)], sums_send)
    departed(raw_in, raw_send)
    departed(xr.at[pl.ds(0, 3)], x_send)
    departed(bank_r.at[pl.ds(0, 63)], b_send)
    departed(o_gate.at[pl.ds(0, 4 * ROWS - 2 * short)], bulk_send)
    for which, width in enumerate(FIRST):
        @pl.when(core == which)
        def _():
            arrived(o_gate.at[pl.ds(0, ROWS), pl.ds(0, width)], pass_recv.at[0])
            arrived(o_up.at[pl.ds(0, ROWS), pl.ds(0, width)], pass_recv.at[1])
            departed(o_gate.at[pl.ds(0, 2 * ROWS), pl.ds(0, width)], pass_send)


def put_first(gate, up, sgate, sup, router, o_gate, o_up, o_sgate, o_sup, o_router, done, sem):
    me, core = lax.axis_index("zero"), lax.rem(lax.axis_index("bank"), 2)
    pairs = ((gate, o_gate), (up, o_up))

    def block(ref, step, width):
        return ref.at[pl.ds(lax.rem(me + step, 4) * ROWS, ROWS), pl.ds(0, width)]

    done[...] = jnp.zeros_like(done)
    copies = []
    for i, (a, b) in enumerate(pairs):
        for k, step in enumerate((0, 1, 3)):
            copies.append(pltpu.make_async_copy(block(a, step, COLS), block(b, step, COLS), sem.at[4 * i + k]))
    copies.append(pltpu.make_async_copy(router, o_router, sem.at[8]))
    copies.append(pltpu.make_async_copy(sgate, o_sgate, sem.at[9]))
    copies.append(pltpu.make_async_copy(sup, o_sup, sem.at[10]))
    for copy in copies:
        copy.start()
    for which, width in enumerate(FIRST):
        @pl.when(core == which)
        def _():
            far = [
                pltpu.make_async_copy(block(a, 2, width), block(b, 2, width), sem.at[4 * i + 3])
                for i, (a, b) in enumerate(pairs)
            ]
            for copy in far:
                copy.start()
            for copy in far:
                copy.wait()

    for copy in copies:
        copy.wait()


def pass_rest(gate, up, _, far_gate, far_up, send, recv):
    bank = lax.axis_index("bank")
    me = lax.axis_index("zero")
    right, left = lax.rem(me + 1, 4), lax.rem(me + 3, 4)
    barrier = pltpu.get_barrier_semaphore()
    for peer in (right, left):
        pl.semaphore_signal(barrier, inc=1, device_id=(bank, peer), device_id_type=MESH)
    pl.semaphore_wait(barrier, 2)
    for which, width in enumerate(FIRST):
        @pl.when(lax.rem(bank, 2) == which)
        def _():
            copies = []
            for k, (src, dst, owner, dest) in enumerate(((gate, far_gate, left, right), (up, far_up, right, left))):
                copies.append(pltpu.make_async_remote_copy(
                    src_ref=src.at[pl.ds(owner * ROWS, ROWS), pl.ds(width, COLS - width)],
                    dst_ref=dst.at[:, pl.ds(0, COLS - width)],
                    send_sem=send.at[k], recv_sem=recv.at[k],
                    device_id=(bank, dest), device_id_type=MESH,
                ))
            for copy in copies:
                copy.start()
            for copy in copies:
                copy.wait()


def put_rest(far_gate, far_up, in_gate, in_up, o_gate, o_up, sem):
    me, core = lax.axis_index("zero"), lax.rem(lax.axis_index("bank"), 2)
    for which, width in enumerate(FIRST):
        @pl.when(core == which)
        def _():
            copies = [
                pltpu.make_async_copy(
                    a.at[:, pl.ds(0, COLS - width)],
                    b.at[pl.ds(lax.rem(me + 2, 4) * ROWS, ROWS), pl.ds(width, COLS - width)],
                    sem.at[i],
                )
                for i, (a, b) in enumerate(((far_gate, o_gate), (far_up, o_up)))
            ]
            for copy in copies:
                copy.start()
            for copy in copies:
                copy.wait()


def local(w_gate, avg_gate, w_up, avg_up, mix_share, router_weight, router_gain):
    dma, regular = pltpu.SemaphoreType.DMA, pltpu.SemaphoreType.REGULAR
    f32, bf16 = jnp.float32, jnp.bfloat16
    anywhere = pl.BlockSpec(memory_space=pl.ANY)
    in_vmem = pl.BlockSpec(memory_space=pltpu.VMEM)
    results = (
        ((4 * ROWS, COLS), bf16), ((4 * ROWS, COLS), bf16),
        ((1, COLS), f32), ((1, COLS), f32), ((64, RB * 128), bf16),
    )
    held = pl.pallas_call(
        kernel,
        out_shape=tuple(pltpu.VMEM(*r) for r in results),
        in_specs=[anywhere] * 4 + [pl.BlockSpec(memory_space=pltpu.SMEM)] + [anywhere] * 2,
        out_specs=[in_vmem] * 5,
        scratch_shapes=[
            pltpu.VMEM((2, ROWS, COLS), f32),
            pltpu.VMEM((2, ROWS, COLS), f32),
            dma((len(LOADS),)),
            pltpu.VMEM((2, ROWS), f32),
            dma(()),
            pltpu.VMEM((4, 1, WIDTH), f32),
            pltpu.VMEM((4, 1, COLS - WIDTH), f32),
            pltpu.VMEM((4, 1, COLS), f32),
            dma(()),
            dma((3,)),
            pltpu.VMEM((2, RAW, HALF), f32),
            dma(()),
            dma(()),
            dma(()),
            dma((2,)),
            dma((2,)),
            dma(()),
            dma(()),
            dma((2,)),
            pltpu.VMEM((4, 4, 128), f32),
            pltpu.VMEM((64, RB, 128), f32),
            dma(()),
            dma(()),
            dma(()),
            dma(()),
            dma((2,)),
            dma((6,)),
            regular,
            regular,
            regular,
        ],
        compiler_params=pltpu.CompilerParams(
            collective_id=0, has_side_effects=True, vmem_limit_bytes=53 * 1024 * 1024
        ),
        name="mean_and_gather",
    )(
        w_gate[0], avg_gate[0], w_up[0], avg_up[0], mix_share,
        router_weight.T, router_gain[None, :],
    )
    results = tuple(jax.ShapeDtypeStruct(*r) for r in results)
    gate, up, sgate, sup, router, done = pl.pallas_call(
        put_first,
        out_shape=results + (pltpu.VMEM((8, 128), f32),),
        in_specs=[in_vmem] * 5,
        out_specs=[anywhere] * 5 + [in_vmem],
        scratch_shapes=[dma((11,))],
        compiler_params=pltpu.CompilerParams(vmem_limit_bytes=1024 * 1024),
        name="put_first",
    )(*held)
    far = pl.pallas_call(
        pass_rest,
        out_shape=(pltpu.VMEM((ROWS, REST), bf16),) * 2,
        in_specs=[in_vmem] * 3,
        out_specs=[in_vmem] * 2,
        scratch_shapes=[dma((2,)), dma((2,))],
        compiler_params=pltpu.CompilerParams(
            collective_id=1, has_side_effects=True, vmem_limit_bytes=1024 * 1024
        ),
        name="pass_rest",
    )(held[0], held[1], done)
    gate, up = pl.pallas_call(
        put_rest,
        out_shape=results[:2],
        in_specs=[in_vmem] * 2 + [anywhere] * 2,
        out_specs=[anywhere] * 2,
        scratch_shapes=[dma((2,))],
        input_output_aliases={2: 0, 3: 1},
        compiler_params=pltpu.CompilerParams(vmem_limit_bytes=1024 * 1024),
        name="put_rest",
    )(*far, gate, up)
    return gate[None], up[None], sgate, sup, router.T


def solution(mesh):
    placed = (
        P("bank", "zero", None),
        P("bank", "zero", None),
        P("bank", "zero", None),
        P("bank", "zero", None),
        P("bank"),
        P("zero", "bank"),
        P("zero"),
    )
    return jax.shard_map(
        local,
        mesh=mesh,
        in_specs=placed,
        out_specs=(
            P("bank", None, None),
            P("bank", None, None),
            P("bank", None),
            P("bank", None),
            P(),
        ),
        check_vma=False,
    )
```

```python
import jax
import jax.numpy as jnp
from jax import lax
from jax.experimental import pallas as pl
from jax.experimental.pallas import tpu as pltpu
from jax.sharding import PartitionSpec as P

MESH = pl.DeviceIdType.MESH
ROWS = 512
COLS = 1024
WIDTH = 256
HALF = WIDTH // 2
PER = COLS // WIDTH
STEP = 128
RB = 16
SOON = 64
RAW = 320
FIRST = (768, 128)
REST = COLS - min(FIRST)
LOADS = ((0, 0, WIDTH), (0, WIDTH, WIDTH), (0, 2 * WIDTH, 2 * WIDTH), (1, 0, 2 * WIDTH), (1, 2 * WIDTH, 2 * WIDTH))


def kernel(
    w_gate, avg_gate, w_up, avg_up, mix, router_w, router_g,
    o_gate, o_up, o_sgate, o_sup, o_router,
    wide, other, load_sem, router_in, router_sem,
    sums0, sums1, sums2, sums_send, sums_recv, raw_in, raw_send, raw_recv,
    bulk_send, gate_recv, up_recv, late_recv, pass_send, pass_recv,
    xr, bank_r, x_send, x_recv, b_send, twin_recv, y_recv, z_recv, joined, ready, go, opposite,
):
    bank = lax.axis_index("bank")
    me = lax.axis_index("zero")
    right, left, across = lax.rem(me + 1, 4), lax.rem(me + 3, 4), lax.rem(me + 2, 4)
    core = lax.rem(bank, 2)
    yy = lax.rem(bank // 2, 4)
    zz = bank // 8

    def at_bank(z, y, c):
        return (z * 4 + y) * 2 + c

    twin = at_bank(zz, yy, 1 - core)
    y_up, y_down = at_bank(zz, lax.rem(yy + 1, 4), core), at_bank(zz, lax.rem(yy + 3, 4), core)
    z_up, z_down = at_bank(lax.rem(zz + 1, 8), yy, core), at_bank(lax.rem(zz + 7, 8), yy, core)
    outs, scales = (o_gate, o_up), (o_sgate, o_sup)
    w_in, a_in = (w_gate, w_up), (avg_gate, avg_up)

    def remote(src, dst, send, recv, where, who):
        return pltpu.make_async_remote_copy(
            src_ref=src, dst_ref=dst, send_sem=send, recv_sem=recv,
            device_id=(where, who), device_id_type=MESH,
        )

    def arrived(ref, sem):
        remote(ref, ref, sem, sem, bank, right).wait_recv()

    def departed(ref, sem):
        remote(ref, ref, sem, sem, bank, right).wait_send()

    def start_load(k):
        m, first, count = LOADS[k]
        cols = pl.ds(first, count)
        pltpu.make_async_copy(w_in[m].at[:, cols], wide.at[m, :, cols], load_sem.at[k]).start()
        pltpu.make_async_copy(a_in[m].at[:, cols], other.at[m, :, cols], load_sem.at[k]).start()

    def loaded(k):
        both = pl.ds(0, 2 * LOADS[k][2])
        pltpu.make_async_copy(w_gate.at[:, both], wide.at[0, :, both], load_sem.at[k]).wait()

    start_load(0)
    start_load(1)

    barrier = pltpu.get_barrier_semaphore()
    lead = jnp.logical_and(core == 1, me == 0)
    beside = (y_up, y_down, z_up, z_down)

    def greet(where, who):
        pl.semaphore_signal(barrier, inc=1, device_id=(where, who), device_id_type=MESH)

    @pl.when(core == 0)
    def _():
        for peer in (right, left):
            greet(bank, peer)

    for step in range(1, 4):
        @pl.when(jnp.logical_and(core == 1, me + step < 4))
        def _():
            greet(bank, lax.rem(me + step, 4))

    @pl.when(lead)
    def _():
        for where in beside:
            greet(where, 0)

    for i in range(1, 4):
        @pl.when(jnp.logical_and(core == 1, me == i))
        def _():
            pl.semaphore_wait(barrier, i)
            for j in range(i):
                pl.semaphore_signal(joined, inc=1, device_id=(bank, j), device_id_type=MESH)

    share = jnp.full((8, WIDTH), mix[0], jnp.float32)
    rest = 1.0 - share

    def mixed(c):
        m, cols = c // PER, pl.ds((c % PER) * WIDTH, WIDTH)

        def step(i, acc):
            for k in range(STEP // 8):
                rows = pl.ds(pl.multiple_of(i * STEP + 8 * k, 8), 8)
                fresh = share * wide[m, rows, cols] + rest * other[m, rows, cols]
                wide[m, rows, cols] = fresh
                acc[k % 4] += fresh * fresh
            return acc

        acc = lax.fori_loop(0, ROWS // STEP, step, [jnp.zeros((8, WIDTH), jnp.float32)] * 4)
        return jnp.sum((acc[0] + acc[1]) + (acc[2] + acc[3]), axis=0, keepdims=True)

    peers = (across, right, left)

    def share_sums(buf, k, peers=peers):
        for peer in peers:
            remote(buf.at[me], buf.at[me], sums_send, sums_recv.at[k], bank, peer).start()

    def totals(buf, k):
        arrived(buf.at[pl.ds(0, 3)], sums_recv.at[k])
        return jnp.sqrt(((buf[0] + buf[1]) + buf[2]) + buf[3])

    loaded(0)
    sums0[me] = mixed(0)
    start_load(2)
    start_load(3)
    start_load(4)
    pltpu.make_async_copy(router_w, router_in.at[pl.ds(0, 1)], router_sem).start()
    pltpu.make_async_copy(router_g, router_in.at[pl.ds(1, 1)], router_sem).start()

    @pl.when(core == 0)
    def _():
        pl.semaphore_wait(barrier, 2)
        pl.semaphore_signal(opposite, inc=1, device_id=(bank, right), device_id_type=MESH)

    for i in range(3):
        @pl.when(jnp.logical_and(core == 1, me == i))
        def _():
            pl.semaphore_wait(joined, 3 - i)

    share_sums(sums0, 0, (right, left))

    def send_raw(first, count):
        rows = pl.ds(first, count)
        for side, dest in enumerate((right, left)):
            remote(wide.at[0, rows, pl.ds(0, HALF)], raw_in.at[side, rows], raw_send, raw_recv, bank, dest).start()

    send_raw(0, SOON)

    @pl.when(core == 0)
    def _():
        pl.semaphore_wait(opposite, 1)

    share_sums(sums0, 0, (across,))
    send_raw(SOON, RAW // 2 - SOON)
    loaded(1)
    sums1[me, :, pl.ds(0, WIDTH)] = mixed(1)
    loaded(2)
    for c in range(2, PER):
        sums1[me, :, pl.ds((c - 1) * WIDTH, WIDTH)] = mixed(c)
    share_sums(sums1, 1)
    send_raw(RAW // 2, RAW // 2)
    for k in (3, 4):
        loaded(k)
        for c in (2 * k - 2, 2 * k - 1):
            sums2[me, :, pl.ds((c - PER) * WIDTH, WIDTH)] = mixed(c)
    share_sums(sums2, 2)

    pltpu.make_async_copy(w_gate.at[pl.ds(0, 2), pl.ds(0, ROWS)], router_in, router_sem).wait()
    prod = router_in[0:1, :] * router_in[1:2, :]
    for k in range(4):
        xr[me, pl.ds(k, 1), :] = prod[:, k * 128 : (k + 1) * 128]
    for peer in peers:
        remote(xr.at[me], xr.at[me], x_send, x_recv, bank, peer).start()

    def where_at(c, owner):
        return outs[c // PER].at[pl.ds(owner * ROWS, ROWS), pl.ds((c % PER) * WIDTH, WIDTH)]

    def normalised(c):
        cols = pl.ds((c % PER) * WIDTH, WIDTH)
        inverse = jnp.broadcast_to(1.0 / scales[c // PER][:, cols], (16, WIDTH))

        def step(i, carry):
            for k in range(STEP // 16):
                rows = pl.ds(pl.multiple_of(i * STEP + 16 * k, 16), 16)
                outs[c // PER][pl.ds(pl.multiple_of(me * ROWS + i * STEP + 16 * k, 16), 16), cols] = (
                    wide[c // PER, rows, cols] * inverse
                ).astype(jnp.bfloat16)
            return carry

        lax.fori_loop(0, ROWS // STEP, step, 0)

    def send_both(block, from_left, from_right):
        remote(block, block, bulk_send, from_left, bank, right).start()
        remote(block, block, bulk_send, from_right, bank, left).start()

    o_sgate[:, pl.ds(0, WIDTH)] = totals(sums0, 0)
    normalised(0)
    send_both(o_gate.at[pl.ds(me * ROWS, ROWS), pl.ds(HALF, HALF)], gate_recv.at[0], gate_recv.at[1])
    send_both(o_gate.at[pl.ds(me * ROWS + RAW, ROWS - RAW), pl.ds(0, HALF)], gate_recv.at[0], gate_recv.at[1])
    o_sgate[:, pl.ds(WIDTH, COLS - WIDTH)] = totals(sums1, 1)
    for c in range(1, PER):
        normalised(c)
        send_both(where_at(c, me), gate_recv.at[0], gate_recv.at[1])
    o_sup[...] = totals(sums2, 2)
    for c in range(PER, 2 * PER):
        normalised(c)
        send_both(where_at(c, me), late_recv, up_recv.at[0 if c < 2 * PER - 1 else 1])

    @pl.when(jnp.logical_and(core == 0, me == 0))
    def _():
        greet(twin, 0)

    @pl.when(lead)
    def _():
        pl.semaphore_wait(barrier, 5)
        for where in beside:
            pl.semaphore_signal(ready, inc=1, device_id=(where, 0), device_id_type=MESH)
        pl.semaphore_wait(ready, 4)
        for j in range(1, 4):
            pl.semaphore_signal(go, inc=1, device_id=(bank, j), device_id_type=MESH)
        for j in range(4):
            pl.semaphore_signal(go, inc=1, device_id=(twin, j), device_id_type=MESH)

    @pl.when(jnp.logical_not(lead))
    def _():
        pl.semaphore_wait(go, 1)

    arrived(xr.at[pl.ds(0, 3)], x_recv)
    for k in range(4):
        bank_r[bank, pl.ds(4 * k, 4), :] = xr[k]

    def push(first, count, dest, recv):
        block = bank_r.at[pl.ds(first, count)]
        remote(block, block, b_send, recv, dest, me).start()

    def got(count, recv):
        arrived(bank_r.at[pl.ds(0, count)], recv)

    push(bank, 1, twin, twin_recv)
    got(1, twin_recv)
    pair = at_bank(zz, yy, 0)
    push(pair, 2, y_up, y_recv.at[0])
    push(pair, 2, y_down, y_recv.at[1])
    got(2, y_recv.at[0])
    push(at_bank(zz, lax.rem(yy + 3, 4), 0), 2, y_up, y_recv.at[1])
    got(4, y_recv.at[1])
    push(zz * 8, 8, z_up, z_recv.at[0])
    push(zz * 8, 8, z_down, z_recv.at[3])
    for k in range(1, 4):
        got(8, z_recv.at[k - 1])
        push(lax.rem(zz + 8 - k, 8) * 8, 8, z_up, z_recv.at[k if k < 3 else 5])
        if k < 3:
            got(8, z_recv.at[k + 2])
            push(lax.rem(zz + k, 8) * 8, 8, z_down, z_recv.at[k + 3])
    got(16, z_recv.at[5])
    for k in range(RB):
        o_router[:, k * 128 : (k + 1) * 128] = bank_r[:, k, :].astype(jnp.bfloat16)

    arrived(raw_in, raw_recv)
    inverse = jnp.broadcast_to(1.0 / o_sgate[:, pl.ds(0, HALF)], (16, HALF))
    for side, owner in enumerate((left, right)):
        for k in range(RAW // 16):
            o_gate[pl.ds(pl.multiple_of(owner * ROWS + 16 * k, 16), 16), pl.ds(0, HALF)] = (
                raw_in[side, pl.ds(16 * k, 16), :] * inverse
            ).astype(jnp.bfloat16)

    short = RAW * HALF // COLS
    arrived(o_gate.at[pl.ds(0, ROWS - short)], gate_recv.at[0])
    for which, width in enumerate(FIRST):
        @pl.when(core == which)
        def _():
            block = o_gate.at[pl.ds(left * ROWS, ROWS), pl.ds(0, width)]
            remote(block, block, pass_send, pass_recv.at[0], bank, right).start()
            for k, (first, end) in enumerate(((0, COLS - WIDTH), (COLS - WIDTH, COLS))):
                arrived(o_up.at[pl.ds(0, ROWS), pl.ds(first, end - first)], up_recv.at[k])
                if first < width:
                    block = o_up.at[pl.ds(right * ROWS, ROWS), pl.ds(first, min(end, width) - first)]
                    remote(block, block, pass_send, pass_recv.at[1], bank, left).start()

    arrived(o_gate.at[pl.ds(0, ROWS - short)], gate_recv.at[1])
    arrived(o_up.at[pl.ds(0, ROWS)], late_recv)
    departed(raw_in.at[0, pl.ds(0, 48)], sums_send)
    departed(raw_in, raw_send)
    departed(xr.at[pl.ds(0, 3)], x_send)
    departed(bank_r.at[pl.ds(0, 63)], b_send)
    departed(o_gate.at[pl.ds(0, 4 * ROWS - 2 * short)], bulk_send)
    for which, width in enumerate(FIRST):
        @pl.when(core == which)
        def _():
            arrived(o_gate.at[pl.ds(0, ROWS), pl.ds(0, width)], pass_recv.at[0])
            arrived(o_up.at[pl.ds(0, ROWS), pl.ds(0, width)], pass_recv.at[1])
            departed(o_gate.at[pl.ds(0, 2 * ROWS), pl.ds(0, width)], pass_send)


def put_first(gate, up, sgate, sup, router, o_gate, o_up, o_sgate, o_sup, o_router, done, sem):
    me, core = lax.axis_index("zero"), lax.rem(lax.axis_index("bank"), 2)
    pairs = ((gate, o_gate), (up, o_up))

    def block(ref, step, width):
        return ref.at[pl.ds(lax.rem(me + step, 4) * ROWS, ROWS), pl.ds(0, width)]

    done[...] = jnp.zeros_like(done)
    copies = []
    for i, (a, b) in enumerate(pairs):
        for k, step in enumerate((0, 1, 3)):
            copies.append(pltpu.make_async_copy(block(a, step, COLS), block(b, step, COLS), sem.at[4 * i + k]))
    copies.append(pltpu.make_async_copy(router, o_router, sem.at[8]))
    copies.append(pltpu.make_async_copy(sgate, o_sgate, sem.at[9]))
    copies.append(pltpu.make_async_copy(sup, o_sup, sem.at[10]))
    for copy in copies:
        copy.start()
    for which, width in enumerate(FIRST):
        @pl.when(core == which)
        def _():
            far = [
                pltpu.make_async_copy(block(a, 2, width), block(b, 2, width), sem.at[4 * i + 3])
                for i, (a, b) in enumerate(pairs)
            ]
            for copy in far:
                copy.start()
            for copy in far:
                copy.wait()

    for copy in copies:
        copy.wait()


def pass_rest(gate, up, _, far_gate, far_up, send, recv):
    bank = lax.axis_index("bank")
    me = lax.axis_index("zero")
    right, left = lax.rem(me + 1, 4), lax.rem(me + 3, 4)
    barrier = pltpu.get_barrier_semaphore()
    for peer in (right, left):
        pl.semaphore_signal(barrier, inc=1, device_id=(bank, peer), device_id_type=MESH)
    pl.semaphore_wait(barrier, 2)
    for which, width in enumerate(FIRST):
        @pl.when(lax.rem(bank, 2) == which)
        def _():
            copies = []
            for k, (src, dst, owner, dest) in enumerate(((gate, far_gate, left, right), (up, far_up, right, left))):
                copies.append(pltpu.make_async_remote_copy(
                    src_ref=src.at[pl.ds(owner * ROWS, ROWS), pl.ds(width, COLS - width)],
                    dst_ref=dst.at[:, pl.ds(0, COLS - width)],
                    send_sem=send.at[k], recv_sem=recv.at[k],
                    device_id=(bank, dest), device_id_type=MESH,
                ))
            for copy in copies:
                copy.start()
            for copy in copies:
                copy.wait()


def put_rest(far_gate, far_up, in_gate, in_up, o_gate, o_up, sem):
    me, core = lax.axis_index("zero"), lax.rem(lax.axis_index("bank"), 2)
    for which, width in enumerate(FIRST):
        @pl.when(core == which)
        def _():
            copies = [
                pltpu.make_async_copy(
                    a.at[:, pl.ds(0, COLS - width)],
                    b.at[pl.ds(lax.rem(me + 2, 4) * ROWS, ROWS), pl.ds(width, COLS - width)],
                    sem.at[i],
                )
                for i, (a, b) in enumerate(((far_gate, o_gate), (far_up, o_up)))
            ]
            for copy in copies:
                copy.start()
            for copy in copies:
                copy.wait()


def local(w_gate, avg_gate, w_up, avg_up, mix_share, router_weight, router_gain):
    dma, regular = pltpu.SemaphoreType.DMA, pltpu.SemaphoreType.REGULAR
    f32, bf16 = jnp.float32, jnp.bfloat16
    anywhere = pl.BlockSpec(memory_space=pl.ANY)
    in_vmem = pl.BlockSpec(memory_space=pltpu.VMEM)
    results = (
        ((4 * ROWS, COLS), bf16), ((4 * ROWS, COLS), bf16),
        ((1, COLS), f32), ((1, COLS), f32), ((64, RB * 128), bf16),
    )
    held = pl.pallas_call(
        kernel,
        out_shape=tuple(pltpu.VMEM(*r) for r in results),
        in_specs=[anywhere] * 4 + [pl.BlockSpec(memory_space=pltpu.SMEM)] + [anywhere] * 2,
        out_specs=[in_vmem] * 5,
        scratch_shapes=[
            pltpu.VMEM((2, ROWS, COLS), f32),
            pltpu.VMEM((2, ROWS, COLS), f32),
            dma((len(LOADS),)),
            pltpu.VMEM((2, ROWS), f32),
            dma(()),
            pltpu.VMEM((4, 1, WIDTH), f32),
            pltpu.VMEM((4, 1, COLS - WIDTH), f32),
            pltpu.VMEM((4, 1, COLS), f32),
            dma(()),
            dma((3,)),
            pltpu.VMEM((2, RAW, HALF), f32),
            dma(()),
            dma(()),
            dma(()),
            dma((2,)),
            dma((2,)),
            dma(()),
            dma(()),
            dma((2,)),
            pltpu.VMEM((4, 4, 128), f32),
            pltpu.VMEM((64, RB, 128), f32),
            dma(()),
            dma(()),
            dma(()),
            dma(()),
            dma((2,)),
            dma((6,)),
            regular,
            regular,
            regular,
            regular,
        ],
        compiler_params=pltpu.CompilerParams(
            collective_id=0, has_side_effects=True, vmem_limit_bytes=53 * 1024 * 1024
        ),
        name="mean_and_gather",
    )(
        w_gate[0], avg_gate[0], w_up[0], avg_up[0], mix_share,
        router_weight.T, router_gain[None, :],
    )
    results = tuple(jax.ShapeDtypeStruct(*r) for r in results)
    gate, up, sgate, sup, router, done = pl.pallas_call(
        put_first,
        out_shape=results + (pltpu.VMEM((8, 128), f32),),
        in_specs=[in_vmem] * 5,
        out_specs=[anywhere] * 5 + [in_vmem],
        scratch_shapes=[dma((11,))],
        compiler_params=pltpu.CompilerParams(vmem_limit_bytes=1024 * 1024),
        name="put_first",
    )(*held)
    far = pl.pallas_call(
        pass_rest,
        out_shape=(pltpu.VMEM((ROWS, REST), bf16),) * 2,
        in_specs=[in_vmem] * 3,
        out_specs=[in_vmem] * 2,
        scratch_shapes=[dma((2,)), dma((2,))],
        compiler_params=pltpu.CompilerParams(
            collective_id=1, has_side_effects=True, vmem_limit_bytes=1024 * 1024
        ),
        name="pass_rest",
    )(held[0], held[1], done)
    gate, up = pl.pallas_call(
        put_rest,
        out_shape=results[:2],
        in_specs=[in_vmem] * 2 + [anywhere] * 2,
        out_specs=[anywhere] * 2,
        scratch_shapes=[dma((2,))],
        input_output_aliases={2: 0, 3: 1},
        compiler_params=pltpu.CompilerParams(vmem_limit_bytes=1024 * 1024),
        name="put_rest",
    )(*far, gate, up)
    return gate[None], up[None], sgate, sup, router.T


def solution(mesh):
    placed = (
        P("bank", "zero", None),
        P("bank", "zero", None),
        P("bank", "zero", None),
        P("bank", "zero", None),
        P("bank"),
        P("zero", "bank"),
        P("zero"),
    )
    return jax.shard_map(
        local,
        mesh=mesh,
        in_specs=placed,
        out_specs=(
            P("bank", None, None),
            P("bank", None, None),
            P("bank", None),
            P("bank", None),
            P(),
        ),
        check_vma=False,
    )
```

```python
import jax
import jax.numpy as jnp
from jax import lax
from jax.experimental import pallas as pl
from jax.experimental.pallas import tpu as pltpu
from jax.sharding import PartitionSpec as P

MESH = pl.DeviceIdType.MESH
ROWS = 512
COLS = 1024
WIDTH = 256
HALF = WIDTH // 2
PER = COLS // WIDTH
STEP = 128
RB = 16
RAW = 320
FIRST = (768, 0)
REST = COLS - min(FIRST)
LOADS = ((0, 0, WIDTH), (0, WIDTH, WIDTH), (0, 2 * WIDTH, 2 * WIDTH), (1, 0, 2 * WIDTH), (1, 2 * WIDTH, 2 * WIDTH))


def kernel(
    w_gate, avg_gate, w_up, avg_up, mix, router_w, router_g,
    o_gate, o_up, o_sgate, o_sup, o_router,
    wide, other, load_sem, router_in, router_sem,
    sums0, sums1, sums2, sums_send, sums_recv, raw_in, raw_send, raw_recv,
    bulk_send, gate_recv, up_recv, late_recv, pass_send, pass_recv,
    xr, bank_r, x_send, x_recv, b_send, twin_recv, y_recv, z_recv, joined, ready, go,
):
    bank = lax.axis_index("bank")
    me = lax.axis_index("zero")
    right, left, across = lax.rem(me + 1, 4), lax.rem(me + 3, 4), lax.rem(me + 2, 4)
    core = lax.rem(bank, 2)
    yy = lax.rem(bank // 2, 4)
    zz = bank // 8

    def at_bank(z, y, c):
        return (z * 4 + y) * 2 + c

    twin = at_bank(zz, yy, 1 - core)
    y_up, y_down = at_bank(zz, lax.rem(yy + 1, 4), core), at_bank(zz, lax.rem(yy + 3, 4), core)
    z_up, z_down = at_bank(lax.rem(zz + 1, 8), yy, core), at_bank(lax.rem(zz + 7, 8), yy, core)
    outs, scales = (o_gate, o_up), (o_sgate, o_sup)
    w_in, a_in = (w_gate, w_up), (avg_gate, avg_up)

    def remote(src, dst, send, recv, where, who):
        return pltpu.make_async_remote_copy(
            src_ref=src, dst_ref=dst, send_sem=send, recv_sem=recv,
            device_id=(where, who), device_id_type=MESH,
        )

    def arrived(ref, sem):
        remote(ref, ref, sem, sem, bank, right).wait_recv()

    def departed(ref, sem):
        remote(ref, ref, sem, sem, bank, right).wait_send()

    def start_load(k, pieces=1):
        m, first, count = LOADS[k]
        cols = pl.ds(first, count)
        for p in range(pieces):
            rows = pl.ds(p * ROWS // pieces, ROWS // pieces)
            pltpu.make_async_copy(w_in[m].at[rows, cols], wide.at[m, rows, cols], load_sem.at[k]).start()
            pltpu.make_async_copy(a_in[m].at[rows, cols], other.at[m, rows, cols], load_sem.at[k]).start()

    def loaded(k):
        both = pl.ds(0, 2 * LOADS[k][2])
        pltpu.make_async_copy(w_gate.at[:, both], wide.at[0, :, both], load_sem.at[k]).wait()

    start_load(0, 4)

    barrier = pltpu.get_barrier_semaphore()
    lead = jnp.logical_and(core == 1, me == 0)
    beside = (y_up, y_down, z_up, z_down)

    def greet(where, who):
        pl.semaphore_signal(barrier, inc=1, device_id=(where, who), device_id_type=MESH)

    @pl.when(core == 0)
    def _():
        for peer in (across, right, left):
            greet(bank, peer)

    for step in range(1, 4):
        @pl.when(jnp.logical_and(core == 1, me + step < 4))
        def _():
            greet(bank, lax.rem(me + step, 4))

    @pl.when(lead)
    def _():
        for where in beside:
            greet(where, 0)

    for i in range(1, 4):
        @pl.when(jnp.logical_and(core == 1, me == i))
        def _():
            pl.semaphore_wait(barrier, i)
            for j in range(i):
                pl.semaphore_signal(joined, inc=1, device_id=(bank, j), device_id_type=MESH)

    share = jnp.full((8, WIDTH), mix[0], jnp.float32)
    rest = 1.0 - share

    def mixed(c):
        m, cols = c // PER, pl.ds((c % PER) * WIDTH, WIDTH)

        def step(i, acc):
            for k in range(STEP // 8):
                rows = pl.ds(pl.multiple_of(i * STEP + 8 * k, 8), 8)
                fresh = share * wide[m, rows, cols] + rest * other[m, rows, cols]
                wide[m, rows, cols] = fresh
                acc[k % 4] += fresh * fresh
            return acc

        acc = lax.fori_loop(0, ROWS // STEP, step, [jnp.zeros((8, WIDTH), jnp.float32)] * 4)
        return jnp.sum((acc[0] + acc[1]) + (acc[2] + acc[3]), axis=0, keepdims=True)

    peers = (across, right, left)

    def share_sums(buf, k):
        for peer in peers:
            remote(buf.at[me], buf.at[me], sums_send, sums_recv.at[k], bank, peer).start()

    def totals(buf, k):
        arrived(buf.at[pl.ds(0, 3)], sums_recv.at[k])
        return jnp.sqrt(((buf[0] + buf[1]) + buf[2]) + buf[3])

    loaded(0)
    start_load(1)
    start_load(2)
    start_load(3)
    start_load(4)
    sums0[me] = mixed(0)
    pltpu.make_async_copy(router_w, router_in.at[pl.ds(0, 1)], router_sem).start()
    pltpu.make_async_copy(router_g, router_in.at[pl.ds(1, 1)], router_sem).start()

    @pl.when(core == 0)
    def _():
        pl.semaphore_wait(barrier, 3)

    for i in range(3):
        @pl.when(jnp.logical_and(core == 1, me == i))
        def _():
            pl.semaphore_wait(joined, 3 - i)

    share_sums(sums0, 0)

    def send_raw(k):
        rows = pl.ds(k * RAW // 2, RAW // 2)
        for side, dest in enumerate((right, left)):
            remote(wide.at[0, rows, pl.ds(0, HALF)], raw_in.at[side, rows], raw_send, raw_recv, bank, dest).start()

    send_raw(0)
    loaded(1)
    sums1[me, :, pl.ds(0, WIDTH)] = mixed(1)
    loaded(2)
    for c in range(2, PER):
        sums1[me, :, pl.ds((c - 1) * WIDTH, WIDTH)] = mixed(c)
    share_sums(sums1, 1)
    send_raw(1)
    for k in (3, 4):
        loaded(k)
        for c in (2 * k - 2, 2 * k - 1):
            sums2[me, :, pl.ds((c - PER) * WIDTH, WIDTH)] = mixed(c)
    share_sums(sums2, 2)

    pltpu.make_async_copy(w_gate.at[pl.ds(0, 2), pl.ds(0, ROWS)], router_in, router_sem).wait()
    prod = router_in[0:1, :] * router_in[1:2, :]
    for k in range(4):
        xr[me, pl.ds(k, 1), :] = prod[:, k * 128 : (k + 1) * 128]
    for peer in peers:
        remote(xr.at[me], xr.at[me], x_send, x_recv, bank, peer).start()

    def where_at(c, owner):
        return outs[c // PER].at[pl.ds(owner * ROWS, ROWS), pl.ds((c % PER) * WIDTH, WIDTH)]

    def normalised(c):
        cols = pl.ds((c % PER) * WIDTH, WIDTH)
        inverse = jnp.broadcast_to(1.0 / scales[c // PER][:, cols], (16, WIDTH))

        def step(i, carry):
            for k in range(STEP // 16):
                rows = pl.ds(pl.multiple_of(i * STEP + 16 * k, 16), 16)
                outs[c // PER][pl.ds(pl.multiple_of(me * ROWS + i * STEP + 16 * k, 16), 16), cols] = (
                    wide[c // PER, rows, cols] * inverse
                ).astype(jnp.bfloat16)
            return carry

        lax.fori_loop(0, ROWS // STEP, step, 0)

    def send_both(block, from_left, from_right):
        remote(block, block, bulk_send, from_left, bank, right).start()
        remote(block, block, bulk_send, from_right, bank, left).start()

    o_sgate[:, pl.ds(0, WIDTH)] = totals(sums0, 0)
    normalised(0)
    send_both(o_gate.at[pl.ds(me * ROWS, ROWS), pl.ds(HALF, HALF)], gate_recv.at[0], gate_recv.at[1])
    send_both(o_gate.at[pl.ds(me * ROWS + RAW, ROWS - RAW), pl.ds(0, HALF)], gate_recv.at[0], gate_recv.at[1])
    o_sgate[:, pl.ds(WIDTH, COLS - WIDTH)] = totals(sums1, 1)
    for c in range(1, PER):
        normalised(c)
        send_both(where_at(c, me), gate_recv.at[0], gate_recv.at[1])
    o_sup[...] = totals(sums2, 2)
    for c in range(PER, 2 * PER):
        normalised(c)
        send_both(where_at(c, me), late_recv, up_recv.at[0 if c < 2 * PER - 1 else 1])

    @pl.when(jnp.logical_and(core == 0, me == 0))
    def _():
        greet(twin, 0)

    @pl.when(lead)
    def _():
        pl.semaphore_wait(barrier, 5)
        for where in beside:
            pl.semaphore_signal(ready, inc=1, device_id=(where, 0), device_id_type=MESH)
        pl.semaphore_wait(ready, 4)
        for j in range(1, 4):
            pl.semaphore_signal(go, inc=1, device_id=(bank, j), device_id_type=MESH)
        for j in range(4):
            pl.semaphore_signal(go, inc=1, device_id=(twin, j), device_id_type=MESH)

    @pl.when(jnp.logical_not(lead))
    def _():
        pl.semaphore_wait(go, 1)

    arrived(xr.at[pl.ds(0, 3)], x_recv)
    for k in range(4):
        bank_r[bank, pl.ds(4 * k, 4), :] = xr[k]

    def push(first, count, dest, recv):
        block = bank_r.at[pl.ds(first, count)]
        remote(block, block, b_send, recv, dest, me).start()

    def got(count, recv):
        arrived(bank_r.at[pl.ds(0, count)], recv)

    push(bank, 1, twin, twin_recv)
    got(1, twin_recv)
    pair = at_bank(zz, yy, 0)
    push(pair, 2, y_up, y_recv.at[0])
    push(pair, 2, y_down, y_recv.at[1])
    got(2, y_recv.at[0])
    push(at_bank(zz, lax.rem(yy + 3, 4), 0), 2, y_up, y_recv.at[1])
    got(4, y_recv.at[1])
    push(zz * 8, 8, z_up, z_recv.at[0])
    push(zz * 8, 8, z_down, z_recv.at[3])
    for k in range(1, 4):
        got(8, z_recv.at[k - 1])
        push(lax.rem(zz + 8 - k, 8) * 8, 8, z_up, z_recv.at[k if k < 3 else 5])
        if k < 3:
            got(8, z_recv.at[k + 2])
            push(lax.rem(zz + k, 8) * 8, 8, z_down, z_recv.at[k + 3])
    got(16, z_recv.at[5])
    for k in range(RB):
        o_router[:, k * 128 : (k + 1) * 128] = bank_r[:, k, :].astype(jnp.bfloat16)

    arrived(raw_in, raw_recv)
    inverse = jnp.broadcast_to(1.0 / o_sgate[:, pl.ds(0, HALF)], (16, HALF))
    for side, owner in enumerate((left, right)):
        for k in range(RAW // 16):
            o_gate[pl.ds(pl.multiple_of(owner * ROWS + 16 * k, 16), 16), pl.ds(0, HALF)] = (
                raw_in[side, pl.ds(16 * k, 16), :] * inverse
            ).astype(jnp.bfloat16)

    short = RAW * HALF // COLS
    arrived(o_gate.at[pl.ds(0, ROWS - short)], gate_recv.at[0])
    for which, width in enumerate(FIRST):
        @pl.when(core == which)
        def _():
            if width:
                block = o_gate.at[pl.ds(left * ROWS, ROWS), pl.ds(0, width)]
                remote(block, block, pass_send, pass_recv.at[0], bank, right).start()
            for k, (first, end) in enumerate(((0, COLS - WIDTH), (COLS - WIDTH, COLS))):
                arrived(o_up.at[pl.ds(0, ROWS), pl.ds(first, end - first)], up_recv.at[k])
                if first < width:
                    block = o_up.at[pl.ds(right * ROWS, ROWS), pl.ds(first, min(end, width) - first)]
                    remote(block, block, pass_send, pass_recv.at[1], bank, left).start()

    arrived(o_gate.at[pl.ds(0, ROWS - short)], gate_recv.at[1])
    arrived(o_up.at[pl.ds(0, ROWS)], late_recv)
    departed(raw_in.at[0, pl.ds(0, 48)], sums_send)
    departed(raw_in, raw_send)
    departed(xr.at[pl.ds(0, 3)], x_send)
    departed(bank_r.at[pl.ds(0, 63)], b_send)
    departed(o_gate.at[pl.ds(0, 4 * ROWS - 2 * short)], bulk_send)
    for which, width in enumerate(FIRST):
        if not width:
            continue

        @pl.when(core == which)
        def _():
            arrived(o_gate.at[pl.ds(0, ROWS), pl.ds(0, width)], pass_recv.at[0])
            arrived(o_up.at[pl.ds(0, ROWS), pl.ds(0, width)], pass_recv.at[1])
            departed(o_gate.at[pl.ds(0, 2 * ROWS), pl.ds(0, width)], pass_send)


def put_first(gate, up, sgate, sup, router, o_gate, o_up, o_sgate, o_sup, o_router, done, sem):
    me, core = lax.axis_index("zero"), lax.rem(lax.axis_index("bank"), 2)
    pairs = ((gate, o_gate), (up, o_up))

    def block(ref, step, width):
        return ref.at[pl.ds(lax.rem(me + step, 4) * ROWS, ROWS), pl.ds(0, width)]

    done[...] = jnp.zeros_like(done)
    copies = []
    for i, (a, b) in enumerate(pairs):
        for k, step in enumerate((0, 1, 3)):
            copies.append(pltpu.make_async_copy(block(a, step, COLS), block(b, step, COLS), sem.at[4 * i + k]))
    copies.append(pltpu.make_async_copy(router, o_router, sem.at[8]))
    copies.append(pltpu.make_async_copy(sgate, o_sgate, sem.at[9]))
    copies.append(pltpu.make_async_copy(sup, o_sup, sem.at[10]))
    for copy in copies:
        copy.start()
    for which, width in enumerate(FIRST):
        if not width:
            continue

        @pl.when(core == which)
        def _():
            far = [
                pltpu.make_async_copy(block(a, 2, width), block(b, 2, width), sem.at[4 * i + 3])
                for i, (a, b) in enumerate(pairs)
            ]
            for copy in far:
                copy.start()
            for copy in far:
                copy.wait()

    for copy in copies:
        copy.wait()


def pass_rest(gate, up, _, far_gate, far_up, send, recv):
    bank = lax.axis_index("bank")
    me = lax.axis_index("zero")
    right, left = lax.rem(me + 1, 4), lax.rem(me + 3, 4)
    barrier = pltpu.get_barrier_semaphore()
    for peer in (right, left):
        pl.semaphore_signal(barrier, inc=1, device_id=(bank, peer), device_id_type=MESH)
    pl.semaphore_wait(barrier, 2)
    for which, width in enumerate(FIRST):
        @pl.when(lax.rem(bank, 2) == which)
        def _():
            copies = []
            for k, (src, dst, owner, dest) in enumerate(((gate, far_gate, left, right), (up, far_up, right, left))):
                copies.append(pltpu.make_async_remote_copy(
                    src_ref=src.at[pl.ds(owner * ROWS, ROWS), pl.ds(width, COLS - width)],
                    dst_ref=dst.at[:, pl.ds(0, COLS - width)],
                    send_sem=send.at[k], recv_sem=recv.at[k],
                    device_id=(bank, dest), device_id_type=MESH,
                ))
            for copy in copies:
                copy.start()
            for copy in copies:
                copy.wait()


def put_rest(far_gate, far_up, in_gate, in_up, o_gate, o_up, sem):
    me, core = lax.axis_index("zero"), lax.rem(lax.axis_index("bank"), 2)
    for which, width in enumerate(FIRST):
        @pl.when(core == which)
        def _():
            copies = [
                pltpu.make_async_copy(
                    a.at[:, pl.ds(0, COLS - width)],
                    b.at[pl.ds(lax.rem(me + 2, 4) * ROWS, ROWS), pl.ds(width, COLS - width)],
                    sem.at[i],
                )
                for i, (a, b) in enumerate(((far_gate, o_gate), (far_up, o_up)))
            ]
            for copy in copies:
                copy.start()
            for copy in copies:
                copy.wait()


def local(w_gate, avg_gate, w_up, avg_up, mix_share, router_weight, router_gain):
    dma, regular = pltpu.SemaphoreType.DMA, pltpu.SemaphoreType.REGULAR
    f32, bf16 = jnp.float32, jnp.bfloat16
    anywhere = pl.BlockSpec(memory_space=pl.ANY)
    in_vmem = pl.BlockSpec(memory_space=pltpu.VMEM)
    results = (
        ((4 * ROWS, COLS), bf16), ((4 * ROWS, COLS), bf16),
        ((1, COLS), f32), ((1, COLS), f32), ((64, RB * 128), bf16),
    )
    held = pl.pallas_call(
        kernel,
        out_shape=tuple(pltpu.VMEM(*r) for r in results),
        in_specs=[anywhere] * 4 + [pl.BlockSpec(memory_space=pltpu.SMEM)] + [anywhere] * 2,
        out_specs=[in_vmem] * 5,
        scratch_shapes=[
            pltpu.VMEM((2, ROWS, COLS), f32),
            pltpu.VMEM((2, ROWS, COLS), f32),
            dma((len(LOADS),)),
            pltpu.VMEM((2, ROWS), f32),
            dma(()),
            pltpu.VMEM((4, 1, WIDTH), f32),
            pltpu.VMEM((4, 1, COLS - WIDTH), f32),
            pltpu.VMEM((4, 1, COLS), f32),
            dma(()),
            dma((3,)),
            pltpu.VMEM((2, RAW, HALF), f32),
            dma(()),
            dma(()),
            dma(()),
            dma((2,)),
            dma((2,)),
            dma(()),
            dma(()),
            dma((2,)),
            pltpu.VMEM((4, 4, 128), f32),
            pltpu.VMEM((64, RB, 128), f32),
            dma(()),
            dma(()),
            dma(()),
            dma(()),
            dma((2,)),
            dma((6,)),
            regular,
            regular,
            regular,
        ],
        compiler_params=pltpu.CompilerParams(
            collective_id=0, has_side_effects=True, vmem_limit_bytes=53 * 1024 * 1024
        ),
        name="mean_and_gather",
    )(
        w_gate[0], avg_gate[0], w_up[0], avg_up[0], mix_share,
        router_weight.T, router_gain[None, :],
    )
    results = tuple(jax.ShapeDtypeStruct(*r) for r in results)
    gate, up, sgate, sup, router, done = pl.pallas_call(
        put_first,
        out_shape=results + (pltpu.VMEM((8, 128), f32),),
        in_specs=[in_vmem] * 5,
        out_specs=[anywhere] * 5 + [in_vmem],
        scratch_shapes=[dma((11,))],
        compiler_params=pltpu.CompilerParams(vmem_limit_bytes=1024 * 1024),
        name="put_first",
    )(*held)
    far = pl.pallas_call(
        pass_rest,
        out_shape=(pltpu.VMEM((ROWS, REST), bf16),) * 2,
        in_specs=[in_vmem] * 3,
        out_specs=[in_vmem] * 2,
        scratch_shapes=[dma((2,)), dma((2,))],
        compiler_params=pltpu.CompilerParams(
            collective_id=1, has_side_effects=True, vmem_limit_bytes=1024 * 1024
        ),
        name="pass_rest",
    )(held[0], held[1], done)
    gate, up = pl.pallas_call(
        put_rest,
        out_shape=results[:2],
        in_specs=[in_vmem] * 2 + [anywhere] * 2,
        out_specs=[anywhere] * 2,
        scratch_shapes=[dma((2,))],
        input_output_aliases={2: 0, 3: 1},
        compiler_params=pltpu.CompilerParams(vmem_limit_bytes=1024 * 1024),
        name="put_rest",
    )(*far, gate, up)
    return gate[None], up[None], sgate, sup, router.T


def solution(mesh):
    placed = (
        P("bank", "zero", None),
        P("bank", "zero", None),
        P("bank", "zero", None),
        P("bank", "zero", None),
        P("bank"),
        P("zero", "bank"),
        P("zero"),
    )
    return jax.shard_map(
        local,
        mesh=mesh,
        in_specs=placed,
        out_specs=(
            P("bank", None, None),
            P("bank", None, None),
            P("bank", None),
            P("bank", None),
            P(),
        ),
        check_vma=False,
    )
```

```python
import jax
import jax.numpy as jnp
from jax import lax
from jax.experimental import pallas as pl
from jax.experimental.pallas import tpu as pltpu
from jax.sharding import PartitionSpec as P

MESH = pl.DeviceIdType.MESH
ROWS = 512
COLS = 1024
WIDTH = 256
HALF = WIDTH // 2
PER = COLS // WIDTH
STEP = 128
RB = 16
RAW = 320
FIRST = (768, 0)
REST = COLS - min(FIRST)
LOADS = ((0, 0, WIDTH), (0, WIDTH, WIDTH), (0, 2 * WIDTH, 2 * WIDTH), (1, 0, 2 * WIDTH), (1, 2 * WIDTH, 2 * WIDTH))


def kernel(
    w_gate, avg_gate, w_up, avg_up, mix, router_w, router_g,
    o_gate, o_up, o_sgate, o_sup, o_router,
    wide, other, load_sem, router_in, router_sem,
    sums0, sums1, sums2, sums_send, sums_recv, raw_in, raw_send, raw_recv,
    bulk_send, gate_recv, up_recv, late_recv, pass_send, pass_recv,
    xr, bank_r, x_send, x_recv, b_send, twin_recv, y_recv, z_recv, joined, ready, go,
):
    bank = lax.axis_index("bank")
    me = lax.axis_index("zero")
    right, left, across = lax.rem(me + 1, 4), lax.rem(me + 3, 4), lax.rem(me + 2, 4)
    core = lax.rem(bank, 2)
    yy = lax.rem(bank // 2, 4)
    zz = bank // 8

    def at_bank(z, y, c):
        return (z * 4 + y) * 2 + c

    twin = at_bank(zz, yy, 1 - core)
    y_up, y_down = at_bank(zz, lax.rem(yy + 1, 4), core), at_bank(zz, lax.rem(yy + 3, 4), core)
    z_up, z_down = at_bank(lax.rem(zz + 1, 8), yy, core), at_bank(lax.rem(zz + 7, 8), yy, core)
    outs, scales = (o_gate, o_up), (o_sgate, o_sup)
    w_in, a_in = (w_gate, w_up), (avg_gate, avg_up)

    def remote(src, dst, send, recv, where, who):
        return pltpu.make_async_remote_copy(
            src_ref=src, dst_ref=dst, send_sem=send, recv_sem=recv,
            device_id=(where, who), device_id_type=MESH,
        )

    def arrived(ref, sem):
        remote(ref, ref, sem, sem, bank, right).wait_recv()

    def departed(ref, sem):
        remote(ref, ref, sem, sem, bank, right).wait_send()

    def start_load(k, pieces=1):
        m, first, count = LOADS[k]
        cols = pl.ds(first, count)
        for p in range(pieces):
            rows = pl.ds(p * ROWS // pieces, ROWS // pieces)
            pltpu.make_async_copy(w_in[m].at[rows, cols], wide.at[m, rows, cols], load_sem.at[k]).start()
            pltpu.make_async_copy(a_in[m].at[rows, cols], other.at[m, rows, cols], load_sem.at[k]).start()

    def loaded(k):
        both = pl.ds(0, 2 * LOADS[k][2])
        pltpu.make_async_copy(w_gate.at[:, both], wide.at[0, :, both], load_sem.at[k]).wait()


    barrier = pltpu.get_barrier_semaphore()
    lead = jnp.logical_and(core == 1, me == 0)
    beside = (y_up, y_down, z_up, z_down)

    def greet(where, who):
        pl.semaphore_signal(barrier, inc=1, device_id=(where, who), device_id_type=MESH)

    @pl.when(core == 0)
    def _():
        for peer in (across, right, left):
            greet(bank, peer)

    for step in range(1, 4):
        @pl.when(jnp.logical_and(core == 1, me + step < 4))
        def _():
            greet(bank, lax.rem(me + step, 4))

    @pl.when(lead)
    def _():
        for where in beside:
            greet(where, 0)

    start_load(0, 4)

    for i in range(1, 4):
        @pl.when(jnp.logical_and(core == 1, me == i))
        def _():
            pl.semaphore_wait(barrier, i)
            for j in range(i):
                pl.semaphore_signal(joined, inc=1, device_id=(bank, j), device_id_type=MESH)

    share = jnp.full((8, WIDTH), mix[0], jnp.float32)
    rest = 1.0 - share

    def mixed(c):
        m, cols = c // PER, pl.ds((c % PER) * WIDTH, WIDTH)

        def step(i, acc):
            for k in range(STEP // 8):
                rows = pl.ds(pl.multiple_of(i * STEP + 8 * k, 8), 8)
                fresh = share * wide[m, rows, cols] + rest * other[m, rows, cols]
                wide[m, rows, cols] = fresh
                acc[k % 4] += fresh * fresh
            return acc

        acc = lax.fori_loop(0, ROWS // STEP, step, [jnp.zeros((8, WIDTH), jnp.float32)] * 4)
        return jnp.sum((acc[0] + acc[1]) + (acc[2] + acc[3]), axis=0, keepdims=True)

    peers = (across, right, left)

    def share_sums(buf, k):
        for peer in peers:
            remote(buf.at[me], buf.at[me], sums_send, sums_recv.at[k], bank, peer).start()

    def totals(buf, k):
        arrived(buf.at[pl.ds(0, 3)], sums_recv.at[k])
        return jnp.sqrt(((buf[0] + buf[1]) + buf[2]) + buf[3])

    loaded(0)
    start_load(1)
    start_load(2)
    start_load(3)
    start_load(4)
    sums0[me] = mixed(0)
    pltpu.make_async_copy(router_w, router_in.at[pl.ds(0, 1)], router_sem).start()
    pltpu.make_async_copy(router_g, router_in.at[pl.ds(1, 1)], router_sem).start()

    @pl.when(core == 0)
    def _():
        pl.semaphore_wait(barrier, 3)

    for i in range(3):
        @pl.when(jnp.logical_and(core == 1, me == i))
        def _():
            pl.semaphore_wait(joined, 3 - i)

    share_sums(sums0, 0)

    def send_raw(k):
        rows = pl.ds(k * RAW // 2, RAW // 2)
        for side, dest in enumerate((right, left)):
            remote(wide.at[0, rows, pl.ds(0, HALF)], raw_in.at[side, rows], raw_send, raw_recv, bank, dest).start()

    send_raw(0)
    loaded(1)
    sums1[me, :, pl.ds(0, WIDTH)] = mixed(1)
    loaded(2)
    for c in range(2, PER):
        sums1[me, :, pl.ds((c - 1) * WIDTH, WIDTH)] = mixed(c)
    share_sums(sums1, 1)
    send_raw(1)
    for k in (3, 4):
        loaded(k)
        for c in (2 * k - 2, 2 * k - 1):
            sums2[me, :, pl.ds((c - PER) * WIDTH, WIDTH)] = mixed(c)
    share_sums(sums2, 2)

    pltpu.make_async_copy(w_gate.at[pl.ds(0, 2), pl.ds(0, ROWS)], router_in, router_sem).wait()
    prod = router_in[0:1, :] * router_in[1:2, :]
    for k in range(4):
        xr[me, pl.ds(k, 1), :] = prod[:, k * 128 : (k + 1) * 128]
    for peer in peers:
        remote(xr.at[me], xr.at[me], x_send, x_recv, bank, peer).start()

    def where_at(c, owner):
        return outs[c // PER].at[pl.ds(owner * ROWS, ROWS), pl.ds((c % PER) * WIDTH, WIDTH)]

    def normalised(c):
        cols = pl.ds((c % PER) * WIDTH, WIDTH)
        inverse = jnp.broadcast_to(1.0 / scales[c // PER][:, cols], (16, WIDTH))

        def step(i, carry):
            for k in range(STEP // 16):
                rows = pl.ds(pl.multiple_of(i * STEP + 16 * k, 16), 16)
                outs[c // PER][pl.ds(pl.multiple_of(me * ROWS + i * STEP + 16 * k, 16), 16), cols] = (
                    wide[c // PER, rows, cols] * inverse
                ).astype(jnp.bfloat16)
            return carry

        lax.fori_loop(0, ROWS // STEP, step, 0)

    def send_both(block, from_left, from_right):
        remote(block, block, bulk_send, from_left, bank, right).start()
        remote(block, block, bulk_send, from_right, bank, left).start()

    o_sgate[:, pl.ds(0, WIDTH)] = totals(sums0, 0)
    normalised(0)
    send_both(o_gate.at[pl.ds(me * ROWS, ROWS), pl.ds(HALF, HALF)], gate_recv.at[0], gate_recv.at[1])
    send_both(o_gate.at[pl.ds(me * ROWS + RAW, ROWS - RAW), pl.ds(0, HALF)], gate_recv.at[0], gate_recv.at[1])
    o_sgate[:, pl.ds(WIDTH, COLS - WIDTH)] = totals(sums1, 1)
    for c in range(1, PER):
        normalised(c)
        send_both(where_at(c, me), gate_recv.at[0], gate_recv.at[1])
    o_sup[...] = totals(sums2, 2)
    for c in range(PER, 2 * PER):
        normalised(c)
        send_both(where_at(c, me), late_recv, up_recv.at[0 if c < 2 * PER - 1 else 1])

    @pl.when(jnp.logical_and(core == 0, me == 0))
    def _():
        greet(twin, 0)

    @pl.when(lead)
    def _():
        pl.semaphore_wait(barrier, 5)
        for where in beside:
            pl.semaphore_signal(ready, inc=1, device_id=(where, 0), device_id_type=MESH)
        pl.semaphore_wait(ready, 4)
        for j in range(1, 4):
            pl.semaphore_signal(go, inc=1, device_id=(bank, j), device_id_type=MESH)
        for j in range(4):
            pl.semaphore_signal(go, inc=1, device_id=(twin, j), device_id_type=MESH)

    @pl.when(jnp.logical_not(lead))
    def _():
        pl.semaphore_wait(go, 1)

    arrived(xr.at[pl.ds(0, 3)], x_recv)
    for k in range(4):
        bank_r[bank, pl.ds(4 * k, 4), :] = xr[k]

    def push(first, count, dest, recv):
        block = bank_r.at[pl.ds(first, count)]
        remote(block, block, b_send, recv, dest, me).start()

    def got(count, recv):
        arrived(bank_r.at[pl.ds(0, count)], recv)

    push(bank, 1, twin, twin_recv)
    got(1, twin_recv)
    pair = at_bank(zz, yy, 0)
    push(pair, 2, y_up, y_recv.at[0])
    push(pair, 2, y_down, y_recv.at[1])
    got(2, y_recv.at[0])
    push(at_bank(zz, lax.rem(yy + 3, 4), 0), 2, y_up, y_recv.at[1])
    got(4, y_recv.at[1])
    push(zz * 8, 8, z_up, z_recv.at[0])
    push(zz * 8, 8, z_down, z_recv.at[3])
    for k in range(1, 4):
        got(8, z_recv.at[k - 1])
        push(lax.rem(zz + 8 - k, 8) * 8, 8, z_up, z_recv.at[k if k < 3 else 5])
        if k < 3:
            got(8, z_recv.at[k + 2])
            push(lax.rem(zz + k, 8) * 8, 8, z_down, z_recv.at[k + 3])
    got(16, z_recv.at[5])
    for k in range(RB):
        o_router[:, k * 128 : (k + 1) * 128] = bank_r[:, k, :].astype(jnp.bfloat16)

    arrived(raw_in, raw_recv)
    inverse = jnp.broadcast_to(1.0 / o_sgate[:, pl.ds(0, HALF)], (16, HALF))
    for side, owner in enumerate((left, right)):
        for k in range(RAW // 16):
            o_gate[pl.ds(pl.multiple_of(owner * ROWS + 16 * k, 16), 16), pl.ds(0, HALF)] = (
                raw_in[side, pl.ds(16 * k, 16), :] * inverse
            ).astype(jnp.bfloat16)

    short = RAW * HALF // COLS
    arrived(o_gate.at[pl.ds(0, ROWS - short)], gate_recv.at[0])
    for which, width in enumerate(FIRST):
        @pl.when(core == which)
        def _():
            if width:
                block = o_gate.at[pl.ds(left * ROWS, ROWS), pl.ds(0, width)]
                remote(block, block, pass_send, pass_recv.at[0], bank, right).start()
            for k, (first, end) in enumerate(((0, COLS - WIDTH), (COLS - WIDTH, COLS))):
                arrived(o_up.at[pl.ds(0, ROWS), pl.ds(first, end - first)], up_recv.at[k])
                if first < width:
                    block = o_up.at[pl.ds(right * ROWS, ROWS), pl.ds(first, min(end, width) - first)]
                    remote(block, block, pass_send, pass_recv.at[1], bank, left).start()

    arrived(o_gate.at[pl.ds(0, ROWS - short)], gate_recv.at[1])
    arrived(o_up.at[pl.ds(0, ROWS)], late_recv)
    departed(raw_in.at[0, pl.ds(0, 48)], sums_send)
    departed(raw_in, raw_send)
    departed(xr.at[pl.ds(0, 3)], x_send)
    departed(bank_r.at[pl.ds(0, 63)], b_send)
    departed(o_gate.at[pl.ds(0, 4 * ROWS - 2 * short)], bulk_send)
    for which, width in enumerate(FIRST):
        if not width:
            continue

        @pl.when(core == which)
        def _():
            arrived(o_gate.at[pl.ds(0, ROWS), pl.ds(0, width)], pass_recv.at[0])
            arrived(o_up.at[pl.ds(0, ROWS), pl.ds(0, width)], pass_recv.at[1])
            departed(o_gate.at[pl.ds(0, 2 * ROWS), pl.ds(0, width)], pass_send)


def put_first(gate, up, sgate, sup, router, o_gate, o_up, o_sgate, o_sup, o_router, done, sem):
    me, core = lax.axis_index("zero"), lax.rem(lax.axis_index("bank"), 2)
    pairs = ((gate, o_gate), (up, o_up))

    def block(ref, step, width):
        return ref.at[pl.ds(lax.rem(me + step, 4) * ROWS, ROWS), pl.ds(0, width)]

    done[...] = jnp.zeros_like(done)
    copies = []
    for i, (a, b) in enumerate(pairs):
        for k, step in enumerate((0, 1, 3)):
            copies.append(pltpu.make_async_copy(block(a, step, COLS), block(b, step, COLS), sem.at[4 * i + k]))
    copies.append(pltpu.make_async_copy(router, o_router, sem.at[8]))
    copies.append(pltpu.make_async_copy(sgate, o_sgate, sem.at[9]))
    copies.append(pltpu.make_async_copy(sup, o_sup, sem.at[10]))
    for copy in copies:
        copy.start()
    for which, width in enumerate(FIRST):
        if not width:
            continue

        @pl.when(core == which)
        def _():
            far = [
                pltpu.make_async_copy(block(a, 2, width), block(b, 2, width), sem.at[4 * i + 3])
                for i, (a, b) in enumerate(pairs)
            ]
            for copy in far:
                copy.start()
            for copy in far:
                copy.wait()

    for copy in copies:
        copy.wait()


def pass_rest(gate, up, _, far_gate, far_up, send, recv):
    bank = lax.axis_index("bank")
    me = lax.axis_index("zero")
    right, left = lax.rem(me + 1, 4), lax.rem(me + 3, 4)
    barrier = pltpu.get_barrier_semaphore()
    for peer in (right, left):
        pl.semaphore_signal(barrier, inc=1, device_id=(bank, peer), device_id_type=MESH)
    pl.semaphore_wait(barrier, 2)
    for which, width in enumerate(FIRST):
        @pl.when(lax.rem(bank, 2) == which)
        def _():
            copies = []
            for k, (src, dst, owner, dest) in enumerate(((gate, far_gate, left, right), (up, far_up, right, left))):
                copies.append(pltpu.make_async_remote_copy(
                    src_ref=src.at[pl.ds(owner * ROWS, ROWS), pl.ds(width, COLS - width)],
                    dst_ref=dst.at[:, pl.ds(0, COLS - width)],
                    send_sem=send.at[k], recv_sem=recv.at[k],
                    device_id=(bank, dest), device_id_type=MESH,
                ))
            for copy in copies:
                copy.start()
            for copy in copies:
                copy.wait()


def put_rest(far_gate, far_up, in_gate, in_up, o_gate, o_up, sem):
    me, core = lax.axis_index("zero"), lax.rem(lax.axis_index("bank"), 2)
    for which, width in enumerate(FIRST):
        @pl.when(core == which)
        def _():
            copies = [
                pltpu.make_async_copy(
                    a.at[:, pl.ds(0, COLS - width)],
                    b.at[pl.ds(lax.rem(me + 2, 4) * ROWS, ROWS), pl.ds(width, COLS - width)],
                    sem.at[i],
                )
                for i, (a, b) in enumerate(((far_gate, o_gate), (far_up, o_up)))
            ]
            for copy in copies:
                copy.start()
            for copy in copies:
                copy.wait()


def local(w_gate, avg_gate, w_up, avg_up, mix_share, router_weight, router_gain):
    dma, regular = pltpu.SemaphoreType.DMA, pltpu.SemaphoreType.REGULAR
    f32, bf16 = jnp.float32, jnp.bfloat16
    anywhere = pl.BlockSpec(memory_space=pl.ANY)
    in_vmem = pl.BlockSpec(memory_space=pltpu.VMEM)
    results = (
        ((4 * ROWS, COLS), bf16), ((4 * ROWS, COLS), bf16),
        ((1, COLS), f32), ((1, COLS), f32), ((64, RB * 128), bf16),
    )
    held = pl.pallas_call(
        kernel,
        out_shape=tuple(pltpu.VMEM(*r) for r in results),
        in_specs=[anywhere] * 4 + [pl.BlockSpec(memory_space=pltpu.SMEM)] + [anywhere] * 2,
        out_specs=[in_vmem] * 5,
        scratch_shapes=[
            pltpu.VMEM((2, ROWS, COLS), f32),
            pltpu.VMEM((2, ROWS, COLS), f32),
            dma((len(LOADS),)),
            pltpu.VMEM((2, ROWS), f32),
            dma(()),
            pltpu.VMEM((4, 1, WIDTH), f32),
            pltpu.VMEM((4, 1, COLS - WIDTH), f32),
            pltpu.VMEM((4, 1, COLS), f32),
            dma(()),
            dma((3,)),
            pltpu.VMEM((2, RAW, HALF), f32),
            dma(()),
            dma(()),
            dma(()),
            dma((2,)),
            dma((2,)),
            dma(()),
            dma(()),
            dma((2,)),
            pltpu.VMEM((4, 4, 128), f32),
            pltpu.VMEM((64, RB, 128), f32),
            dma(()),
            dma(()),
            dma(()),
            dma(()),
            dma((2,)),
            dma((6,)),
            regular,
            regular,
            regular,
        ],
        compiler_params=pltpu.CompilerParams(
            collective_id=0, has_side_effects=True, vmem_limit_bytes=53 * 1024 * 1024
        ),
        name="mean_and_gather",
    )(
        w_gate[0], avg_gate[0], w_up[0], avg_up[0], mix_share,
        router_weight.T, router_gain[None, :],
    )
    results = tuple(jax.ShapeDtypeStruct(*r) for r in results)
    gate, up, sgate, sup, router, done = pl.pallas_call(
        put_first,
        out_shape=results + (pltpu.VMEM((8, 128), f32),),
        in_specs=[in_vmem] * 5,
        out_specs=[anywhere] * 5 + [in_vmem],
        scratch_shapes=[dma((11,))],
        compiler_params=pltpu.CompilerParams(vmem_limit_bytes=1024 * 1024),
        name="put_first",
    )(*held)
    far = pl.pallas_call(
        pass_rest,
        out_shape=(pltpu.VMEM((ROWS, REST), bf16),) * 2,
        in_specs=[in_vmem] * 3,
        out_specs=[in_vmem] * 2,
        scratch_shapes=[dma((2,)), dma((2,))],
        compiler_params=pltpu.CompilerParams(
            collective_id=1, has_side_effects=True, vmem_limit_bytes=1024 * 1024
        ),
        name="pass_rest",
    )(held[0], held[1], done)
    gate, up = pl.pallas_call(
        put_rest,
        out_shape=results[:2],
        in_specs=[in_vmem] * 2 + [anywhere] * 2,
        out_specs=[anywhere] * 2,
        scratch_shapes=[dma((2,))],
        input_output_aliases={2: 0, 3: 1},
        compiler_params=pltpu.CompilerParams(vmem_limit_bytes=1024 * 1024),
        name="put_rest",
    )(*far, gate, up)
    return gate[None], up[None], sgate, sup, router.T


def solution(mesh):
    placed = (
        P("bank", "zero", None),
        P("bank", "zero", None),
        P("bank", "zero", None),
        P("bank", "zero", None),
        P("bank"),
        P("zero", "bank"),
        P("zero"),
    )
    return jax.shard_map(
        local,
        mesh=mesh,
        in_specs=placed,
        out_specs=(
            P("bank", None, None),
            P("bank", None, None),
            P("bank", None),
            P("bank", None),
            P(),
        ),
        check_vma=False,
    )
```
